32 devices in a mesh: freq: 4 (over y, x), param: 8 (over z, core).
Axes of the slice: x: 2, y: 2, z: 4, core: 2. Of those that a mesh axis runs over, the one named last changes fastest.
Arguments:
- sources: float32 [4, 420, 1024], P(None, None, ('param', 'freq')), may hold values from -6 to 6
- kernel: bfloat16 [424, 2, 600, 1024], P('freq', None, None, 'param'), may hold values from -0.125 to 0.125
- bin_of_slot: int32 [424], replicated, may hold values from 0 to 420, as said below
Outputs:
- observations: float32 [4, 420, 600], P(None, None, 'freq')
The draws below stay inside these ranges and needn't reach their ends.
Inputs may be any that keep to these rules, and one draw needn't show every extreme that they name: `bin_of_slot`: every bin from 0 to 420 is named by at least one slot; the other slots name bins again.
All inputs are finite; a program needn't handle non-finite values.
Results may differ from the reference program's by a relative error of at most 0.0031.
Values may be sent and summed in bfloat16 or wider, within the bound.
No kernel may reach another device: no remote copies, remote signals or barrier semaphores. Data moves between devices by JAX's collectives and lax.ppermute only.
A program may use at most 128 MiB of HBM per device.

```python
import math
import jax
import jax.numpy as jnp
from jax import lax

NT = 420
NS = 600
SCEN = 4
NFB = 421
SLOTS = 424
NM = 1024


def draw_bin_of_slot(key, part):
    base_key = jax.random.fold_in(key, 7)
    first_key, second_key = jax.random.split(base_key)
    extra = jax.random.randint(first_key, (SLOTS - NFB,), 0, NFB, dtype=jnp.int32)
    listed = jnp.concatenate([jnp.arange(NFB, dtype=jnp.int32), extra])
    order = jax.random.permutation(second_key, SLOTS)
    return listed[order].astype(jnp.int32)


def level_of(stream_key, dims, cuts, least, largest):
    loudness = 1.0
    for axis_at, shards_of in cuts:
        draws = jax.random.uniform(jax.random.fold_in(jax.random.fold_in(stream_key, 6), axis_at), (shards_of,), jnp.float32, least / len(cuts), largest / len(cuts))
        loudness = loudness * jnp.repeat(jnp.exp(draws), dims[axis_at] // shards_of).reshape((-1,) + (1,) * (len(dims) - 1 - axis_at))
    return loudness


def noise(own_key, dims, width, most, cuts=(), held_as=jnp.bfloat16):
    factor_of = level_of(own_key, dims, cuts, -0.22, 0.18) if cuts else 1.0
    drawn = jax.random.normal(own_key, dims, jnp.float32) * width * factor_of
    return jnp.minimum(jnp.maximum(drawn, -most), most).astype(held_as)


def setup_inputs(seed: int = 0) -> dict:
    key_list = jax.random.split(jax.random.key(seed), 4)
    return {
        "sources": noise(key_list[0], (SCEN, NT, NM), 1.0, 6.0, ((2, 32),), jnp.float32),
        "kernel": noise(key_list[1], (SLOTS, 2, NS, NM), (2 * NM) ** -0.5, 0.125, ((0, 4), (3, 8))),
        "bin_of_slot": draw_bin_of_slot(jax.random.fold_in(key_list[3], 71), 0),
    }


def angle_tables(bins, steps, scale):
    times = jnp.arange(steps, dtype=jnp.int32)
    phase = bins[:, None].astype(jnp.int32) * times[None, :] % (2 * steps)
    angle = phase.astype(jnp.float32) * (2.0 * math.pi / (2 * steps))
    return (jnp.cos(angle) * scale, jnp.sin(angle) * scale)

def reference(sources, kernel, bin_of_slot):
    highest = lax.Precision.HIGHEST
    cos_fwd, sin_fwd = angle_tables(bin_of_slot, NT, 1.0 / math.sqrt(NT))
    spec_real = jnp.einsum('st,ctj->scj', cos_fwd, sources, precision=highest).astype(jnp.bfloat16)
    spec_imag = jnp.einsum('st,ctj->scj', -sin_fwd, sources, precision=highest).astype(jnp.bfloat16)

    def respond(items):
        block, real_part, imag_part = items
        real = jnp.dot(real_part, block[0].T, preferred_element_type=jnp.float32) - jnp.dot(imag_part, block[1].T, preferred_element_type=jnp.float32)
        imag = jnp.dot(imag_part, block[0].T, preferred_element_type=jnp.float32) + jnp.dot(real_part, block[1].T, preferred_element_type=jnp.float32)
        return (real, imag)
    resp_real, resp_imag = lax.map(respond, (kernel, spec_real, spec_imag))
    weights = jnp.where((bin_of_slot == 0) | (bin_of_slot == NT), jnp.float32(1.0), jnp.float32(2.0))
    cos_inv, sin_inv = angle_tables(bin_of_slot, NT, 1.0 / math.sqrt(2.0 * (NT + 1)))
    cos_inv = cos_inv * weights[:, None]
    sin_inv = sin_inv * weights[:, None]
    observations = jnp.einsum('st,sck->ctk', cos_inv, resp_real, precision=highest) - jnp.einsum('st,sck->ctk', sin_inv, resp_imag, precision=highest)
    return observations
```

```python
import functools
import math

import jax
import jax.numpy as jnp
import numpy as np
from jax import lax
from jax.experimental import pallas as pl
from jax.experimental.pallas import tpu as pltpu
from jax.sharding import PartitionSpec as P

LANES = 128
BF16, F32, I32 = jnp.bfloat16, jnp.float32, jnp.int32
VMEM = pltpu.VMEM
CHUNK = 8


def up(value, unit):
    return -(-value // unit) * unit


def dot_nt(left, right):
    return lax.dot_general(left, right, (((1,), (1,)), ((), ())), preferred_element_type=F32)


def dot_nn(left, right):
    return jnp.dot(left, right, preferred_element_type=F32)


def halves(value):
    high = value.astype(BF16)
    return high, (value - high.astype(F32)).astype(BF16)


class Plan:
    def __init__(self, mesh, sources, kernel, bin_of_slot):
        self.freq = mesh.shape["freq"]
        self.param = mesh.shape["param"]
        self.pieces = self.param // 2
        self.count, self.steps, self.mine = sources.shape
        self.slots = bin_of_slot.shape[0]
        self.here, _, self.sensors, self.depth = kernel.shape
        self.half = self.count // 2
        self.comps = 2 * self.half
        self.group = LANES // self.comps
        self.groups = -(-self.here // self.group)
        self.block = self.sensors // self.freq
        self.block_pad = up(self.block, 8)
        self.bins = up(self.steps + 1, LANES)
        self.span = -(-self.steps // self.pieces)
        self.span_pad = up(self.span, LANES)
        self.slots_pad = up(self.slots, LANES)
        assert self.here <= LANES and self.depth == self.mine * self.freq
        assert self.freq & (self.freq - 1) == 0 and self.pieces & (self.pieces - 1) == 0

    def tables(self):
        times = np.arange(self.steps)
        rows = times // self.span * self.span_pad + times % self.span
        bins = np.arange(self.steps + 1)
        angle = (times[:, None] * bins[None, :] % (2 * self.steps)) * (math.pi / self.steps)
        table = np.zeros((self.pieces * self.span_pad, 2 * self.bins), np.float64)
        table[rows, : self.steps + 1] = np.cos(angle)
        table[rows, self.bins : self.bins + self.steps + 1] = np.sin(angle)
        high = table.astype(jnp.bfloat16)
        low = (table - high.astype(np.float64)).astype(jnp.bfloat16)
        return high, low


def bin_row(plan, bins_ref, row_ref):
    row_ref[...] = jnp.full(row_ref.shape, -1, I32)
    row_ref[0:1, 0 : plan.slots] = bins_ref[...]
    return row_ref[0:1, :]


def slot_hits(plan, row, shard):
    shift = (-plan.here * shard) % plan.slots_pad
    if shift:
        row = pltpu.roll(row, shift, 1)
    row = row[:, :LANES]
    lane = lax.broadcasted_iota(I32, (1, LANES), 1)
    row = jnp.where(lane < plan.here, row, -1)
    bins = lax.broadcasted_iota(I32, (plan.bins, LANES), 0)
    return jnp.where(bins == row, 1.0, 0.0).astype(BF16)


def forward_kernel(plan, bins_ref, src_ref, high_ref, low_ref, *rest):
    outs, (row_ref, time_ref, send_ref) = rest[: plan.freq], rest[plan.freq :]
    me = lax.axis_index("freq")
    time_ref[...] = jnp.zeros(time_ref.shape, F32)
    for c in range(plan.count):
        for z in range(plan.pieces):
            first = z * plan.span
            size = min(plan.span, plan.steps - first)
            time_ref[
                z * plan.span_pad : z * plan.span_pad + size, c * plan.mine : (c + 1) * plan.mine
            ] = src_ref[c, first : first + size, :]
    rows = plan.count * plan.mine
    high, low = halves(time_ref[...].T[:rows])
    spectrum = (
        dot_nn(high, high_ref[...]) + dot_nn(high, low_ref[...]) + dot_nn(low, high_ref[...])
    )
    scale = 1.0 / math.sqrt(plan.steps)
    both = jnp.concatenate(
        [
            (spectrum[:, : plan.bins] * scale).astype(BF16),
            (spectrum[:, plan.bins :] * -scale).astype(BF16),
        ],
        axis=0,
    )
    row = bin_row(plan, bins_ref, row_ref)
    for shard in range(plan.freq):
        picked = dot_nn(both, slot_hits(plan, row, shard))
        for c in range(plan.count):
            for part in range(2):
                first = part * rows + c * plan.mine
                comp = 2 * (c % plan.half) + part
                value = picked[first : first + plan.mine]
                if comp:
                    value = pltpu.roll(value, comp * plan.group, 1)
                send_ref[shard, 2 * c + part] = value.astype(BF16)
    for k in range(plan.freq):
        outs[k][...] = send_ref[me ^ k]


def response_kernel(plan, first_group, last_group, *refs):
    freq, group = plan.freq, plan.group
    arrived, kern_ref = refs[:freq], refs[freq]
    own_ref, other_ref, buf_ref, spec_ref, rhs_ref, acc_ref, sem_ref = refs[freq + 1 :]
    first = first_group * group
    total = min(last_group * group, plan.here) - first
    chunks = [(at, min(CHUNK, total - at)) for at in range(0, total, CHUNK)]
    copies = [
        pltpu.make_async_copy(
            kern_ref.at[pl.ds(first + at, size)], buf_ref.at[pl.ds(at, size)], sem_ref.at[i]
        )
        for i, (at, size) in enumerate(chunks)
    ]
    for copy in copies:
        copy.start()
    me, core = lax.axis_index("freq"), lax.axis_index("param") % 2
    for k in range(freq):
        at = pl.multiple_of((me ^ k) * plan.mine, plan.mine)
        spec_ref[:, pl.ds(at, plan.mine), :] = arrived[k][...]
    lane = lax.broadcasted_iota(I32, (plan.depth, LANES), 1)
    for g in range(first_group, last_group):
        for side in range(2):
            base = (core ^ side) * plan.comps
            place = (lane // group - g) % plan.comps
            real = spec_ref[base].astype(F32)
            for comp in range(1, plan.comps):
                real = jnp.where(place == comp, spec_ref[base + comp].astype(F32), real)
            imag = jnp.where(
                place % 2 == 0, -pltpu.roll(real, LANES - group, 1), pltpu.roll(real, group, 1)
            )
            cols = slice(side * LANES, (side + 1) * LANES)
            rhs_ref[g - first_group, : plan.depth, cols] = real.astype(BF16)
            rhs_ref[g - first_group, plan.depth :, cols] = imag.astype(BF16)
    within = lax.broadcasted_iota(I32, (2 * plan.depth, 2 * LANES), 1) % group

    def product(g, at, size):
        weights = rhs_ref[g]
        left, right = [], []
        for s in range(size):
            left += [buf_ref[at + s, 0], buf_ref[at + s, 1]]
            right.append(jnp.where(within == (at + s) % group, weights, jnp.zeros_like(weights)))
        return dot_nn(jnp.concatenate(left, axis=1), jnp.concatenate(right, axis=0))

    for g in range(last_group - first_group):
        inside = [(i, at, size) for i, (at, size) in enumerate(chunks) if at // group == g]
        for n, (i, at, size) in enumerate(inside):
            copies[i].wait()
            value = product(g, at, size)
            if n:
                value = acc_ref[...] + value
            if n + 1 < len(inside):
                acc_ref[...] = value
        for f in range(freq):
            rows = value[f * plan.block : (f + 1) * plan.block]
            own_ref[f, g] = rows[:, :LANES]
            other_ref[f, g] = rows[:, LANES:]


def join_kernel(plan, own_ref, other_ref, *outs):
    me = lax.axis_index("freq")
    for k in range(plan.freq):
        outs[k][...] = (own_ref[me ^ k] + other_ref[me ^ k]).astype(BF16)


def inverse_kernel(plan, calls, bins_ref, high_ref, low_ref, *rest):
    freq, group, pad = plan.freq, plan.group, plan.block_pad
    arrived, rest = rest[: calls * freq], rest[calls * freq :]
    outs, (row_ref, hits_ref, joined_ref) = rest[: plan.pieces], rest[plan.pieces :]
    me, piece = lax.axis_index("freq"), lax.axis_index("param") // 2
    row = bin_row(plan, bins_ref, row_ref)
    for shard in range(freq):
        hits_ref[shard] = slot_hits(plan, row, shard)
    lane = lax.broadcasted_iota(I32, (plan.block, LANES), 1)
    joined_ref[...] = jnp.zeros(joined_ref.shape, BF16)
    for k in range(freq):
        tiles = []
        for call in range(calls):
            ref = arrived[call * freq + k]
            tiles += [ref[g].astype(F32) for g in range(ref.shape[0])]
        for comp in range(plan.comps):
            value = jnp.zeros((plan.block, LANES), F32)
            for g, tile in enumerate(tiles):
                value = jnp.where(lane // group == (g + comp) % plan.comps, tile, value)
            if comp:
                value = pltpu.roll(value, LANES - comp * group, 1)
            at = comp * pad
            joined_ref[at : at + plan.block, k * LANES : (k + 1) * LANES] = value.astype(BF16)
    hits = jnp.concatenate([hits_ref[me ^ k] for k in range(freq)], axis=1)
    by_bin = dot_nt(joined_ref[...], hits)
    bins = lax.broadcasted_iota(I32, (1, plan.bins), 1)
    weight = jnp.where((bins == 0) | (bins == plan.steps), 1.0, 2.0) * (
        1.0 / math.sqrt(2.0 * (plan.steps + 1))
    )
    rows = []
    for c in range(plan.half):
        real = by_bin[2 * c * pad : (2 * c + 1) * pad] * weight
        imag = by_bin[(2 * c + 1) * pad : (2 * c + 2) * pad] * -weight
        rows.append(jnp.concatenate([real, imag], axis=1))
    high, low = halves(jnp.concatenate(rows, axis=0))
    for k in range(plan.pieces):
        at = pl.multiple_of((piece ^ k) * plan.span_pad, plan.span_pad)
        table_high = high_ref[pl.ds(at, plan.span_pad), :]
        table_low = low_ref[pl.ds(at, plan.span_pad), :]
        value = dot_nt(high, table_high) + dot_nt(low, table_high) + dot_nt(high, table_low)
        outs[k][...] = value.astype(outs[k].dtype)


def sum_kernel(*refs):
    value = refs[0][...]
    for ref in refs[1:-1]:
        value = value + ref[...].astype(F32)
    refs[-1][...] = value.astype(BF16)


def output_kernel(plan, *refs):
    out_ref = refs[-1]
    piece, core = lax.axis_index("param") // 2, lax.axis_index("param") % 2
    width = plan.span_pad
    time = lax.broadcasted_iota(I32, (plan.steps, plan.pieces * width), 0)
    lane = lax.broadcasted_iota(I32, (plan.steps, plan.pieces * width), 1)
    inside = lane % width
    target = (lane // width ^ piece) * plan.span + inside
    pick = jnp.where((time == target) & (inside < plan.span), 1.0, 0.0).astype(BF16)
    for side in range(2):
        parts = refs[side * plan.pieces : (side + 1) * plan.pieces]
        for c in range(plan.half):
            at = c * plan.block_pad
            value = jnp.concatenate([ref[at : at + plan.block_pad, :] for ref in parts], axis=1)
            out_ref[(core ^ side) * plan.half + c] = dot_nt(pick, value)[:, : plan.block]


def call(body, out_shapes, args, in_specs=None, scratch=(), cost=None, limit=None):
    whole = pl.BlockSpec(memory_space=VMEM)
    return pl.pallas_call(
        body,
        out_shape=out_shapes,
        in_specs=in_specs or [whole] * len(args),
        out_specs=jax.tree.map(lambda _: whole, out_shapes),
        scratch_shapes=list(scratch),
        cost_estimate=cost,
        compiler_params=pltpu.CompilerParams(vmem_limit_bytes=limit),
    )(*args)


def shards(mesh, sources, kernel, bin_of_slot):
    plan = Plan(mesh, sources, kernel, bin_of_slot)
    freq, pieces = plan.freq, plan.pieces
    shape = jax.ShapeDtypeStruct
    high, low = plan.tables()
    bins = bin_of_slot.reshape(1, plan.slots)
    row = VMEM((8, plan.slots_pad), I32)
    whole = pl.BlockSpec(memory_space=VMEM)

    def over_freq(values):
        return [values[0]] + [
            lax.ppermute(values[k], "freq", [(i, i ^ k) for i in range(freq)])
            for k in range(1, freq)
        ]

    def to_piece(value, k):
        pairs = [(2 * z + h, 2 * (z ^ k) + h) for z in range(pieces) for h in range(2)]
        return lax.ppermute(value, "param", pairs)

    def to_core(value):
        return lax.ppermute(value, "param", [(i, i ^ 1) for i in range(plan.param)])

    spectra = call(
        functools.partial(forward_kernel, plan),
        [shape((2 * plan.count, plan.mine, LANES), BF16)] * freq,
        (bins, sources, high, low),
        scratch=[
            row,
            VMEM((pieces * plan.span_pad, up(plan.count * plan.mine, LANES)), F32),
            VMEM((freq, 2 * plan.count, plan.mine, LANES), BF16),
        ],
    )
    arrived = over_freq(spectra)

    middle = -(-plan.groups // 2)
    ranges = [(0, middle), (middle, plan.groups)]
    parts = []
    for begin, end in ranges:
        total = min(end * plan.group, plan.here) - begin * plan.group
        size = shape((freq, end - begin, plan.block, LANES), F32)
        own, other = call(
            functools.partial(response_kernel, plan, begin, end),
            [size, size],
            (*arrived, kernel),
            in_specs=[whole] * freq + [pl.BlockSpec(memory_space=pl.ANY)],
            scratch=[
                VMEM((total, 2, plan.sensors, plan.depth), BF16),
                VMEM((2 * plan.count, plan.depth, LANES), BF16),
                VMEM((end - begin, 2 * plan.depth, 2 * LANES), BF16),
                VMEM((plan.sensors, 2 * LANES), F32),
                pltpu.SemaphoreType.DMA((-(-total // CHUNK),)),
            ],
            cost=pl.CostEstimate(
                flops=total * 2 * plan.sensors * plan.depth * 256,
                bytes_accessed=total * 4 * plan.sensors * plan.depth,
                transcendentals=0,
            ),
            limit=56 * 1024 * 1024,
        )
        summed = call(
            functools.partial(join_kernel, plan),
            [shape((end - begin, plan.block, LANES), BF16)] * freq,
            (own, to_core(other)),
        )
        parts += over_freq(summed)

    rows = plan.half * plan.block_pad
    partial = call(
        functools.partial(inverse_kernel, plan, len(ranges)),
        [shape((rows, plan.span_pad), BF16 if k else F32) for k in range(pieces)],
        (bins, high, low, *parts),
        scratch=[
            row,
            VMEM((freq, plan.bins, LANES), BF16),
            VMEM((plan.comps * plan.block_pad, freq * LANES), BF16),
        ],
    )
    received = [to_piece(partial[k], k) for k in range(1, pieces)]
    piece = call(sum_kernel, shape((rows, plan.span_pad), BF16), (partial[0], *received))
    mine = [piece] + [to_piece(piece, k) for k in range(1, pieces)]
    theirs = [to_core(value) for value in mine]
    return call(
        functools.partial(output_kernel, plan),
        shape((plan.count, plan.steps, plan.block), F32),
        (*mine, *theirs),
    )


def solution(mesh):
    return jax.shard_map(
        functools.partial(shards, mesh),
        mesh=mesh,
        in_specs=(P(None, None, ("param", "freq")), P("freq", None, None, "param"), P()),
        out_specs=P(None, None, "freq"),
        check_vma=False,
    )
```

```python
import functools
import math

import jax
import jax.numpy as jnp
import numpy as np
from jax import lax
from jax.experimental import pallas as pl
from jax.experimental.pallas import tpu as pltpu
from jax.sharding import PartitionSpec as P

LANES = 128
BF16, F32, I32 = jnp.bfloat16, jnp.float32, jnp.int32
VMEM = pltpu.VMEM
MIB = 1024 * 1024
LIMIT = 16 * MIB
FULL = 67043328
ROOM = 10 * MIB + 400 * 1024
CHUNK, EARLY, AHEAD = 8, 5, 3


def up(value, unit):
    return -(-value // unit) * unit


def dot_nt(left, right):
    return lax.dot_general(left, right, (((1,), (1,)), ((), ())), preferred_element_type=F32)


def dot_nn(left, right):
    return jnp.dot(left, right, preferred_element_type=F32)


def halves(value):
    high = value.astype(BF16)
    return high, (value - high.astype(F32)).astype(BF16)


class Plan:
    def __init__(self, mesh, sources, kernel, bin_of_slot):
        self.freq = mesh.shape["freq"]
        self.param = mesh.shape["param"]
        self.pieces = self.param // 2
        self.count, self.steps, self.mine = sources.shape
        self.slots = bin_of_slot.shape[0]
        self.here, _, self.sensors, self.depth = kernel.shape
        self.half = self.count // 2
        self.comps = 2 * self.half
        self.group = LANES // self.comps
        self.groups = -(-self.here // self.group)
        self.block = self.sensors // self.freq
        self.block_pad = up(self.block, 8)
        self.bins = up(self.steps + 1, LANES)
        self.span = -(-self.steps // self.pieces)
        self.span_pad = up(self.span, LANES)
        self.slots_pad = up(self.slots, LANES)
        self.last = self.here - (self.groups - 1) * self.group
        self.fold = self.group // self.last
        self.fold_rows = up(-(-self.block_pad // self.fold), 8)
        self.share_rows = (self.groups - 1) * self.block_pad + self.fold_rows
        self.rows = self.half * self.block_pad
        self.spare = self.span_pad - self.span
        self.base = self.rows
        if self.spare:
            self.cuts = -(-self.span // self.spare)
            while (self.rows - self.base + 16) * self.cuts <= self.base - 16:
                self.base -= 16
        self.tail = self.rows - self.base
        assert self.here <= LANES and self.depth == self.mine * self.freq
        assert self.freq & (self.freq - 1) == 0 and self.pieces & (self.pieces - 1) == 0

    def tables(self):
        times = np.arange(self.steps)
        rows = times // self.span * self.span_pad + times % self.span
        bins = np.arange(self.steps + 1)
        angle = (times[:, None] * bins[None, :] % (2 * self.steps)) * (math.pi / self.steps)
        table = np.zeros((self.pieces * self.span_pad, 2 * self.bins), np.float64)
        table[rows, : self.steps + 1] = np.cos(angle)
        table[rows, self.bins : self.bins + self.steps + 1] = np.sin(angle)
        high = table.astype(jnp.bfloat16)
        low = (table - high.astype(np.float64)).astype(jnp.bfloat16)
        return high, low


def pack(plan, value):
    if not plan.tail:
        return value
    tail, parts = value[plan.base :], []
    for j in range(plan.cuts):
        parts.append(pltpu.roll(tail, (plan.span - plan.spare * j) % plan.span_pad, 1))
    left = plan.base - plan.tail * plan.cuts
    if left:
        parts.append(jnp.zeros((left, plan.span_pad), F32))
    lane = lax.broadcasted_iota(I32, (plan.base, plan.span_pad), 1)
    return jnp.where(lane < plan.span, value[: plan.base], jnp.concatenate(parts, axis=0))


def unpack(plan, value):
    if not plan.tail:
        return value
    tail = jnp.zeros((plan.tail, plan.span_pad), F32)
    lane = lax.broadcasted_iota(I32, tail.shape, 1)
    for j in range(plan.cuts):
        part = value[plan.tail * j : plan.tail * (j + 1)]
        part = pltpu.roll(part, (plan.spare * j - plan.span) % plan.span_pad, 1)
        tail = jnp.where(lane // plan.spare == j, part, tail)
    return jnp.concatenate([value, tail], axis=0)


def bin_row(plan, bins_ref, row_ref):
    row_ref[...] = jnp.full(row_ref.shape, -1, I32)
    row_ref[0:1, 0 : plan.slots] = bins_ref[...]
    return row_ref[0:1, :]


def slot_hits(plan, row, shard):
    shift = (-plan.here * shard) % plan.slots_pad
    if shift:
        row = pltpu.roll(row, shift, 1)
    row = row[:, :LANES]
    lane = lax.broadcasted_iota(I32, (1, LANES), 1)
    row = jnp.where(lane < plan.here, row, -1)
    bins = lax.broadcasted_iota(I32, (plan.bins, LANES), 0)
    return jnp.where(bins == row, 1.0, 0.0).astype(BF16)


def stream(kern_ref, first, size, target, sem_ref, index):
    return pltpu.make_async_copy(
        kern_ref.at[pl.ds(first, size)], target.at[pl.ds(0, size)], sem_ref.at[index]
    )


def forward_kernel(plan, *refs):
    ins, outs, rest = refs[:4], refs[4 : 4 + plan.freq], refs[4 + plan.freq :]
    bins_ref, src_ref, high_ref, low_ref, row_ref, time_ref, send_ref, sem_ref = rest
    copies = [
        pltpu.make_async_copy(source, target, sem_ref.at[i])
        for i, (source, target) in enumerate(zip(ins, rest))
    ]
    for copy in copies:
        copy.start()
    for copy in copies:
        copy.wait()
    me = lax.axis_index("freq")
    time_ref[...] = jnp.zeros(time_ref.shape, F32)
    rows = plan.count * plan.mine
    for z in range(plan.pieces):
        first = z * plan.span
        size = min(plan.span, plan.steps - first)
        at = z * plan.span_pad
        time_ref[:, at : at + size] = src_ref[:, :, first : first + size].reshape(rows, size)
    high, low = halves(time_ref[...])
    spectrum = (
        dot_nn(high, high_ref[...]) + dot_nn(high, low_ref[...]) + dot_nn(low, high_ref[...])
    )
    scale = 1.0 / math.sqrt(plan.steps)
    both = jnp.concatenate(
        [
            (spectrum[:, : plan.bins] * scale).astype(BF16),
            (spectrum[:, plan.bins :] * -scale).astype(BF16),
        ],
        axis=0,
    )
    row = bin_row(plan, bins_ref, row_ref)
    for shard in range(plan.freq):
        picked = dot_nn(both, slot_hits(plan, row, shard))
        for c in range(plan.count):
            for part in range(2):
                first = part * rows + c * plan.mine
                comp = 2 * (c % plan.half) + part
                value = picked[first : first + plan.mine]
                if comp:
                    value = pltpu.roll(value, comp * plan.group, 1)
                send_ref[shard, 2 * c + part] = value.astype(BF16)
    for k in range(plan.freq):
        outs[k][...] = send_ref[me ^ k]


def load_kernel(plan, count, after_ref, bins_ref, kern_ref, out_ref, hits_ref, row_ref, sem_ref):
    starts = range(0, count, CHUNK)
    copies = [
        stream(kern_ref, at, min(CHUNK, count - at), out_ref.at[pl.ds(at, CHUNK)], sem_ref, i)
        for i, at in enumerate(starts)
    ]
    for copy in copies:
        copy.start()
    row = bin_row(plan, bins_ref, row_ref)
    for shard in range(plan.freq):
        hits_ref[shard] = slot_hits(plan, row, shard)
    for copy in copies:
        copy.wait()


def response_kernel(plan, begin, end, held, ahead, *refs):
    freq, group = plan.freq, plan.group
    arrived, refs = refs[:freq], refs[freq:]
    held_refs, kern_ref, refs = refs[: len(held)], refs[len(held)], refs[len(held) + 1 :]
    places = [(ref, at) for ref, size in zip(held_refs, held) for at in range(size)]
    ready = len(places)
    own_ref, other_ref, refs = refs[0], refs[1], refs[2:]
    if ahead:
        ahead_ref, refs = refs[0], refs[1:]
    buf_ref, spec_ref, rhs_ref, sem_ref = refs
    first_group, last_group = begin, end
    first = first_group * group
    total = min(last_group * group, plan.here) - first
    copies, late = {}, []
    for at in range(ready, total, CHUNK):
        size = min(CHUNK, total - at)
        target = buf_ref.at[pl.ds(at - ready, size)]
        copies[at] = stream(kern_ref, first + at, size, target, sem_ref, len(copies))
    for at in range(0, ahead, CHUNK):
        size = min(CHUNK, ahead - at)
        target = ahead_ref.at[pl.ds(at, size)]
        index = len(copies) + len(late)
        late.append(stream(kern_ref, first + total + at, size, target, sem_ref, index))
    for copy in [*copies.values(), *late]:
        copy.start()
    me, core = lax.axis_index("freq"), lax.axis_index("param") % 2
    for k in range(freq):
        at = pl.multiple_of((me ^ k) * plan.mine, plan.mine)
        spec_ref[:, pl.ds(at, plan.mine), :] = arrived[k][...]
    lane = lax.broadcasted_iota(I32, (plan.depth, LANES), 1)
    for g in range(first_group, last_group):
        for side in range(2):
            base = (core ^ side) * plan.comps
            place = (lane // group - g) % plan.comps
            real = spec_ref[base].astype(F32)
            for comp in range(1, plan.comps):
                real = jnp.where(place == comp, spec_ref[base + comp].astype(F32), real)
            imag = jnp.where(
                place % 2 == 0, -pltpu.roll(real, LANES - group, 1), pltpu.roll(real, group, 1)
            )
            cols = slice(side * LANES, (side + 1) * LANES)
            rhs_ref[g - first_group, : plan.depth, cols] = real.astype(BF16)
            rhs_ref[g - first_group, plan.depth :, cols] = imag.astype(BF16)
    within = lax.broadcasted_iota(I32, (2 * plan.depth, 2 * LANES), 1) % group

    def multiply(acc_even, acc_odd):
        accs = (acc_even, acc_odd)

        def push(slot):
            weights = rhs_ref[slot // group]
            pltpu.matmul_push_rhs(
                jnp.where(within == slot % group, weights, jnp.zeros_like(weights)),
                staging_register=slot // 2 % 2,
                mxu_index=slot % 2,
            )

        for acc in accs:
            pltpu.matmul_pop(acc)
        for slot in range(min(2, total)):
            push(slot)
        for slot in range(total):
            if slot + 2 < total:
                push(slot + 2)
            if slot in copies:
                copies[slot].wait()
            ref, at = places[slot] if slot < ready else (buf_ref, slot - ready)
            both = [ref[at, part] for part in range(2)]
            left = jnp.concatenate(both, axis=1)
            if left.shape[0] % 16:
                left = jnp.concatenate([left, left[:8]], axis=0)
            pltpu.matmul_acc_lhs(accs[slot % 2], left, load_staged_rhs=slot // 2 % 2)
            if (slot + 1) % group == 0 or slot + 1 == total:
                g = slot // group
                value = pltpu.matmul_pop(acc_even) + pltpu.matmul_pop(acc_odd)
                for f in range(freq):
                    rows = value[f * plan.block : (f + 1) * plan.block]
                    at = (f * (last_group - first_group) + g) * plan.block_pad
                    own_ref[at : at + plan.block] = rows[:, :LANES]
                    other_ref[at : at + plan.block] = rows[:, LANES:]

    shape = (up(plan.sensors, 16), 2 * LANES)
    pl.run_scoped(multiply, pltpu.ACC(0)(shape, F32), pltpu.ACC(1)(shape, F32))
    for copy in late:
        copy.wait()


def join_kernel(plan, sizes, *refs):
    pairs, outs = refs[: 2 * len(sizes)], refs[2 * len(sizes) :]
    me, pad, fold_rows = lax.axis_index("freq"), plan.block_pad, plan.fold_rows
    lane = lax.broadcasted_iota(I32, (fold_rows, LANES), 1) % plan.group
    for k in range(plan.freq):
        done = 0
        for call_at, size in enumerate(sizes):
            own_ref, other_ref = pairs[2 * call_at : 2 * call_at + 2]
            at = pl.multiple_of((me ^ k) * (size * pad), 8)
            value = own_ref[pl.ds(at, size * pad)] + other_ref[pl.ds(at, size * pad)]
            full = min(size, plan.groups - 1 - done) * pad
            if full:
                outs[k][done * pad : done * pad + full] = value[:full].astype(BF16)
            done += size
        tile, packed = value[full:], jnp.zeros((fold_rows, LANES), F32)
        for j in range(plan.fold):
            part = tile[j * fold_rows : (j + 1) * fold_rows]
            if part.shape[0] < fold_rows:
                rest = jnp.zeros((fold_rows - part.shape[0], LANES), F32)
                part = jnp.concatenate([part, rest], axis=0)
            if j:
                part = pltpu.roll(part, j * plan.last, 1)
            packed = jnp.where(lane // plan.last == j, part, packed)
        outs[k][plan.share_rows - fold_rows :] = packed.astype(BF16)


def inverse_kernel(plan, hits_ref, high_ref, low_ref, *rest):
    freq, group, pad = plan.freq, plan.group, plan.block_pad
    arrived, rest = rest[:freq], rest[freq:]
    outs, (joined_ref,) = rest[: plan.pieces], rest[plan.pieces :]
    me, piece = lax.axis_index("freq"), lax.axis_index("param") // 2
    lane = lax.broadcasted_iota(I32, (pad, LANES), 1)
    real_row = lax.broadcasted_iota(I32, (pad, LANES), 0) < plan.block
    for k in range(freq):
        starts = range(0, (plan.groups - 1) * pad, pad)
        tiles = [arrived[k][at : at + pad].astype(F32) for at in starts]
        packed = arrived[k][plan.share_rows - plan.fold_rows :].astype(F32)
        folds = [packed] + [
            pltpu.roll(packed, LANES - j * plan.last, 1) for j in range(1, plan.fold)
        ]
        tiles.append(jnp.concatenate(folds, axis=0)[:pad])
        for comp in range(plan.comps):
            value = jnp.zeros((pad, LANES), F32)
            for g, tile in enumerate(tiles):
                inside = (lane // group == (g + comp) % plan.comps) & real_row
                value = jnp.where(inside, tile, value)
            if comp:
                value = pltpu.roll(value, LANES - comp * group, 1)
            at = comp * pad
            joined_ref[at : at + pad, k * LANES : (k + 1) * LANES] = value.astype(BF16)
    hits = jnp.concatenate([hits_ref[me ^ k] for k in range(freq)], axis=1)
    by_bin = dot_nt(joined_ref[...], hits)
    bins = lax.broadcasted_iota(I32, (1, plan.bins), 1)
    weight = jnp.where((bins == 0) | (bins == plan.steps), 1.0, 2.0)
    rows = []
    for c in range(plan.half):
        real = by_bin[2 * c * pad : (2 * c + 1) * pad] * weight
        imag = by_bin[(2 * c + 1) * pad : (2 * c + 2) * pad] * -weight
        rows.append(jnp.concatenate([real, imag], axis=1).astype(BF16))
    high = jnp.concatenate(rows, axis=0)
    scale = 1.0 / math.sqrt(2.0 * (plan.steps + 1))
    for k in range(plan.pieces):
        at = pl.multiple_of((piece ^ k) * plan.span_pad, plan.span_pad)
        table_high = high_ref[pl.ds(at, plan.span_pad), :]
        table_low = low_ref[pl.ds(at, plan.span_pad), :]
        value = (dot_nt(high, table_high) + dot_nt(high, table_low)) * scale
        outs[k][...] = pack(plan, value).astype(outs[k].dtype)


def stack_kernel(*refs):
    size = refs[0].shape[0]
    for k, ref in enumerate(refs[:-1]):
        refs[-1][k * size : (k + 1) * size] = ref[...]


def sum_kernel(*refs):
    value = refs[0][...]
    for ref in refs[1:-1]:
        value = value + ref[...].astype(F32)
    refs[-1][...] = value.astype(BF16)


def output_kernel(plan, *refs):
    out_ref = refs[-1]
    piece, core = lax.axis_index("param") // 2, lax.axis_index("param") % 2
    width = plan.span_pad
    time = lax.broadcasted_iota(I32, (plan.steps, plan.pieces * width), 0)
    lane = lax.broadcasted_iota(I32, (plan.steps, plan.pieces * width), 1)
    inside = lane % width
    target = (lane // width ^ piece) * plan.span + inside
    pick = jnp.where((time == target) & (inside < plan.span), 1.0, 0.0).astype(BF16)
    for side in range(2):
        parts = [
            unpack(plan, refs[side][k * plan.base : (k + 1) * plan.base].astype(F32)).astype(BF16)
            for k in range(plan.pieces)
        ]
        value = dot_nt(jnp.concatenate(parts, axis=1), pick)
        for c in range(plan.half):
            at = c * plan.block_pad
            out_ref[:, (core ^ side) * plan.half + c, :] = value[at : at + plan.block]


def cost(flops, moved):
    return pl.CostEstimate(flops=flops, bytes_accessed=moved, transcendentals=0)


def call(body, out_shapes, args, in_specs=None, scratch=(), cost=None, limit=LIMIT):
    whole = pl.BlockSpec(memory_space=VMEM)
    return pl.pallas_call(
        body,
        out_shape=out_shapes,
        in_specs=in_specs or [whole] * len(args),
        out_specs=jax.tree.map(lambda _: whole, out_shapes),
        scratch_shapes=list(scratch),
        cost_estimate=cost,
        compiler_params=pltpu.CompilerParams(vmem_limit_bytes=limit),
    )(*args)


def shards(mesh, sources, kernel, bin_of_slot):
    plan = Plan(mesh, sources, kernel, bin_of_slot)
    freq, pieces = plan.freq, plan.pieces
    shape = jax.ShapeDtypeStruct
    high, low = plan.tables()
    bins = bin_of_slot.reshape(1, plan.slots)
    row = VMEM((8, plan.slots_pad), I32)
    whole = pl.BlockSpec(memory_space=VMEM)

    def over_freq(values):
        return [values[0]] + [
            lax.ppermute(values[k], "freq", [(i, i ^ k) for i in range(freq)])
            for k in range(1, freq)
        ]

    def to_piece(value, k):
        pairs = [(2 * z + h, 2 * (z ^ k) + h) for z in range(pieces) for h in range(2)]
        return lax.ppermute(value, "param", pairs)

    def to_core(value):
        return lax.ppermute(value, "param", [(i, i ^ 1) for i in range(plan.param)])

    middle = -(-plan.groups // 2)
    ranges = [(0, middle), (middle, plan.groups)]
    sizes = [end - begin for begin, end in ranges]
    totals = [min(end * plan.group, plan.here) - begin * plan.group for begin, end in ranges]
    block = (2, plan.sensors, plan.depth)
    early = min(totals[0] // CHUNK, EARLY) * CHUNK

    spectra = call(
        functools.partial(forward_kernel, plan),
        [shape((2 * plan.count, plan.mine, LANES), BF16)] * freq,
        (bins, jnp.transpose(sources, (0, 2, 1)), high, low),
        in_specs=[pl.BlockSpec(memory_space=pltpu.HBM)] * 4,
        scratch=[
            VMEM(bins.shape, I32),
            VMEM((plan.count, plan.mine, plan.steps), F32),
            VMEM(high.shape, BF16),
            VMEM(low.shape, BF16),
            row,
            VMEM((plan.count * plan.mine, pieces * plan.span_pad), F32),
            VMEM((freq, 2 * plan.count, plan.mine, LANES), BF16),
            pltpu.SemaphoreType.DMA((4,)),
        ],
        cost=cost(2 * 10**9, 2 * high.size),
        limit=FULL - ROOM,
    )
    arrived = over_freq(spectra)

    hbm = pl.BlockSpec(memory_space=pltpu.HBM)
    ready, hits = call(
        functools.partial(load_kernel, plan, early),
        [shape((early, *block), BF16), shape((freq, plan.bins, LANES), BF16)],
        (spectra[0], bins, kernel),
        in_specs=[pl.BlockSpec(memory_space=pl.ANY), whole, hbm],
        scratch=[row, pltpu.SemaphoreType.DMA((-(-early // CHUNK),))],
        cost=cost(4 * 10**9, 4 * early * plan.sensors * plan.depth),
    )
    ready = [ready]
    pairs = []
    for index, (begin, end) in enumerate(ranges):
        total, held = totals[index], [array.shape[0] for array in ready]
        rest = total - sum(held)
        ahead = 0 if index else min(totals[1] // CHUNK, AHEAD) * CHUNK
        size = shape((freq * sizes[index] * plan.block_pad, LANES), F32)
        own, other, *later = call(
            functools.partial(response_kernel, plan, begin, end, held, ahead),
            [size, size] + ([shape((ahead, *block), BF16)] if ahead else []),
            (*arrived, *ready, kernel),
            in_specs=[whole] * (freq + len(ready)) + [hbm],
            scratch=[
                VMEM((max(rest, CHUNK), *block), BF16),
                VMEM((2 * plan.count, plan.depth, LANES), BF16),
                VMEM((end - begin, 2 * plan.depth, 2 * LANES), BF16),
                pltpu.SemaphoreType.DMA((-(-rest // CHUNK) + ahead // CHUNK + 1,)),
            ],
            cost=cost(total * 512 * plan.sensors * plan.depth, 4 * total * plan.sensors * plan.depth),
        )
        ready = later
        pairs += [own, to_core(other)]
    joined = call(
        functools.partial(join_kernel, plan, sizes),
        [shape((plan.share_rows, LANES), BF16)] * freq,
        pairs,
    )
    parts = over_freq(joined)

    partial = call(
        functools.partial(inverse_kernel, plan),
        [shape((plan.base, plan.span_pad), BF16 if k else F32) for k in range(pieces)],
        (hits, high, low, *parts),
        scratch=[
            VMEM((plan.comps * plan.block_pad, freq * LANES), BF16),
        ],
    )
    received = [to_piece(partial[k], k) for k in range(1, pieces)]
    piece = call(sum_kernel, shape((plan.base, plan.span_pad), BF16), (partial[0], *received))
    mine = [piece] + [to_piece(piece, k) for k in range(1, pieces)]
    mine = call(stack_kernel, shape((pieces * plan.base, plan.span_pad), BF16), mine)
    theirs = to_core(mine)
    by_sensor = call(
        functools.partial(output_kernel, plan),
        shape((plan.block, plan.count, plan.steps), F32),
        (mine, theirs),
    )
    return jnp.transpose(by_sensor, (1, 2, 0))


def solution(mesh):
    return jax.shard_map(
        functools.partial(shards, mesh),
        mesh=mesh,
        in_specs=(P(None, None, ("param", "freq")), P("freq", None, None, "param"), P()),
        out_specs=P(None, None, "freq"),
        check_vma=False,
    )
```

```python
import functools
import math

import jax
import jax.numpy as jnp
import numpy as np
from jax import lax
from jax.experimental import pallas as pl
from jax.experimental.pallas import tpu as pltpu
from jax.sharding import PartitionSpec as P

LANES = 128
BF16, F32, I32 = jnp.bfloat16, jnp.float32, jnp.int32
VMEM = pltpu.VMEM
MIB = 1024 * 1024
LIMIT = 16 * MIB
FULL = 67043328
ROOM = 10 * MIB + 400 * 1024
CHUNK, EARLY, AHEAD = 8, 5, 2


def up(value, unit):
    return -(-value // unit) * unit


def by_step(refs):
    return [refs[0], *refs[:0:-1]]


def dot_nt(left, right):
    return lax.dot_general(left, right, (((1,), (1,)), ((), ())), preferred_element_type=F32)


def dot_nn(left, right):
    return jnp.dot(left, right, preferred_element_type=F32)


def halves(value):
    high = value.astype(BF16)
    return high, (value - high.astype(F32)).astype(BF16)


class Plan:
    def __init__(self, mesh, sources, kernel, bin_of_slot):
        self.freq = mesh.shape["freq"]
        self.param = mesh.shape["param"]
        self.pieces = self.param // 2
        self.count, self.steps, self.mine = sources.shape
        self.slots = bin_of_slot.shape[0]
        self.here, _, self.sensors, self.depth = kernel.shape
        self.half = self.count // 2
        self.comps = 2 * self.half
        self.group = LANES // self.comps
        self.groups = -(-self.here // self.group)
        self.block = self.sensors // self.freq
        self.block_pad = up(self.block, 8)
        self.bins = up(self.steps + 1, LANES)
        self.span = -(-self.steps // self.pieces)
        self.span_pad = up(self.span, LANES)
        self.slots_pad = up(self.slots, LANES)
        self.last = self.here - (self.groups - 1) * self.group
        self.fold = self.group // self.last
        self.fold_rows = up(-(-self.block_pad // self.fold), 8)
        self.rows = self.half * self.block_pad
        self.spare = self.span_pad - self.span
        self.base = self.rows
        if self.spare:
            self.cuts = -(-self.span // self.spare)
            while (self.rows - self.base + 16) * self.cuts <= self.base - 16:
                self.base -= 16
        self.tail = self.rows - self.base
        assert self.here <= LANES and self.depth == self.mine * self.freq
        assert self.freq & (self.freq - 1) == 0 and self.pieces & (self.pieces - 1) == 0

    def tables(self):
        times = np.arange(self.steps)
        rows = times // self.span * self.span_pad + times % self.span
        bins = np.arange(self.steps + 1)
        angle = (times[:, None] * bins[None, :] % (2 * self.steps)) * (math.pi / self.steps)
        table = np.zeros((self.pieces * self.span_pad, 2 * self.bins), np.float64)
        table[rows, : self.steps + 1] = np.cos(angle)
        table[rows, self.bins : self.bins + self.steps + 1] = np.sin(angle)
        high = table.astype(jnp.bfloat16)
        low = (table - high.astype(np.float64)).astype(jnp.bfloat16)
        return high, low


def pack(plan, value):
    if not plan.tail:
        return value
    tail, parts = value[plan.base :], []
    for j in range(plan.cuts):
        parts.append(pltpu.roll(tail, (plan.span - plan.spare * j) % plan.span_pad, 1))
    left = plan.base - plan.tail * plan.cuts
    if left:
        parts.append(jnp.zeros((left, plan.span_pad), F32))
    lane = lax.broadcasted_iota(I32, (plan.base, plan.span_pad), 1)
    return jnp.where(lane < plan.span, value[: plan.base], jnp.concatenate(parts, axis=0))


def unpack(plan, value):
    if not plan.tail:
        return value
    tail = jnp.zeros((plan.tail, plan.span_pad), F32)
    lane = lax.broadcasted_iota(I32, tail.shape, 1)
    for j in range(plan.cuts):
        part = value[plan.tail * j : plan.tail * (j + 1)]
        part = pltpu.roll(part, (plan.spare * j - plan.span) % plan.span_pad, 1)
        tail = jnp.where(lane // plan.spare == j, part, tail)
    return jnp.concatenate([value, tail], axis=0)


def bin_row(plan, bins_ref, row_ref):
    row_ref[...] = jnp.full(row_ref.shape, -1, I32)
    row_ref[0:1, 0 : plan.slots] = bins_ref[...]
    return row_ref[0:1, :]


def slot_hits(plan, row, shard):
    shift = (-plan.here * shard) % plan.slots_pad
    if shift:
        row = pltpu.roll(row, shift, 1)
    row = row[:, :LANES]
    lane = lax.broadcasted_iota(I32, (1, LANES), 1)
    row = jnp.where(lane < plan.here, row, -1)
    bins = lax.broadcasted_iota(I32, (plan.bins, LANES), 0)
    return jnp.where(bins == row, 1.0, 0.0).astype(BF16)


def stream(kern_ref, first, size, target, sem_ref, index):
    return pltpu.make_async_copy(
        kern_ref.at[pl.ds(first, size)], target.at[pl.ds(0, size)], sem_ref.at[index]
    )


def forward_kernel(plan, *refs):
    ins, outs, rest = refs[:4], refs[4 : 4 + plan.freq], refs[4 + plan.freq :]
    bins_ref, src_ref, high_ref, low_ref, row_ref, time_ref, send_ref, sem_ref = rest
    copies = [
        pltpu.make_async_copy(source, target, sem_ref.at[i])
        for i, (source, target) in enumerate(zip(ins, rest))
    ]
    for copy in copies:
        copy.start()
    for copy in copies:
        copy.wait()
    me = lax.axis_index("freq")
    time_ref[...] = jnp.zeros(time_ref.shape, F32)
    rows = plan.count * plan.mine
    for z in range(plan.pieces):
        first = z * plan.span
        size = min(plan.span, plan.steps - first)
        at = z * plan.span_pad
        time_ref[:, at : at + size] = src_ref[:, :, first : first + size].reshape(rows, size)
    high, low = halves(time_ref[...])
    spectrum = (
        dot_nn(high, high_ref[...]) + dot_nn(high, low_ref[...]) + dot_nn(low, high_ref[...])
    )
    scale = 1.0 / math.sqrt(plan.steps)
    both = jnp.concatenate(
        [
            (spectrum[:, : plan.bins] * scale).astype(BF16),
            (spectrum[:, plan.bins :] * -scale).astype(BF16),
        ],
        axis=0,
    )
    row = bin_row(plan, bins_ref, row_ref)
    for shard in range(plan.freq):
        picked = dot_nn(both, slot_hits(plan, row, shard))
        for c in range(plan.count):
            for part in range(2):
                first = part * rows + c * plan.mine
                comp = 2 * (c % plan.half) + part
                value = picked[first : first + plan.mine]
                if comp:
                    value = pltpu.roll(value, comp * plan.group, 1)
                send_ref[shard, 2 * c + part] = value.astype(BF16)
    for k in range(plan.freq):
        outs[k][...] = send_ref[me ^ k]


def load_kernel(plan, count, after_ref, bins_ref, kern_ref, out_ref, hits_ref, row_ref, sem_ref):
    starts = range(0, count, CHUNK)
    copies = [
        stream(kern_ref, at, min(CHUNK, count - at), out_ref.at[pl.ds(at, CHUNK)], sem_ref, i)
        for i, at in enumerate(starts)
    ]
    for copy in copies:
        copy.start()
    row = bin_row(plan, bins_ref, row_ref)
    for shard in range(plan.freq):
        hits_ref[shard] = slot_hits(plan, row, shard)
    for copy in copies:
        copy.wait()


def response_kernel(plan, begin, end, held, ahead, *refs):
    freq, group = plan.freq, plan.group
    arrived, refs = by_step(refs[:freq]), refs[freq:]
    held_refs, refs = refs[: len(held)], refs[len(held) :]
    if ahead or sum(held) < min(end * group, plan.here) - begin * group:
        kern_ref, refs = refs[0], refs[1:]
    places = [(ref, at) for ref, size in zip(held_refs, held) for at in range(size)]
    ready = len(places)
    own_ref, other_ref, refs = refs[0], refs[1], refs[2:]
    if ahead:
        ahead_ref, refs = refs[0], refs[1:]
    buf_ref, spec_ref, rhs_ref, sem_ref = refs
    first_group, last_group = begin, end
    first = first_group * group
    total = min(last_group * group, plan.here) - first
    copies, late = {}, []
    for at in range(ready, total, CHUNK):
        size = min(CHUNK, total - at)
        target = buf_ref.at[pl.ds(at - ready, size)]
        copies[at] = stream(kern_ref, first + at, size, target, sem_ref, len(copies))
    for at in range(0, ahead, CHUNK):
        size = min(CHUNK, ahead - at)
        target = ahead_ref.at[pl.ds(at, size)]
        index = len(copies) + len(late)
        late.append(stream(kern_ref, first + total + at, size, target, sem_ref, index))
    for copy in [*copies.values(), *late]:
        copy.start()
    me, core = lax.axis_index("freq"), lax.axis_index("param") % 2
    for k in range(freq):
        at = pl.multiple_of((me ^ k) * plan.mine, plan.mine)
        spec_ref[:, pl.ds(at, plan.mine), :] = arrived[k][...]
    lane = lax.broadcasted_iota(I32, (plan.depth, LANES), 1)
    for g in range(first_group, last_group):
        for side in range(2):
            base = (core ^ side) * plan.comps
            place = (lane // group - g) % plan.comps
            real = spec_ref[base].astype(F32)
            for comp in range(1, plan.comps):
                real = jnp.where(place == comp, spec_ref[base + comp].astype(F32), real)
            imag = jnp.where(
                place % 2 == 0, -pltpu.roll(real, LANES - group, 1), pltpu.roll(real, group, 1)
            )
            cols = slice(side * LANES, (side + 1) * LANES)
            rhs_ref[g - first_group, : plan.depth, cols] = real.astype(BF16)
            rhs_ref[g - first_group, plan.depth :, cols] = imag.astype(BF16)
    within = lax.broadcasted_iota(I32, (2 * plan.depth, 2 * LANES), 1) % group

    def multiply(acc_even, acc_odd):
        accs = (acc_even, acc_odd)

        def push(slot):
            weights = rhs_ref[slot // group]
            pltpu.matmul_push_rhs(
                jnp.where(within == slot % group, weights, jnp.zeros_like(weights)),
                staging_register=slot // 2 % 2,
                mxu_index=slot % 2,
            )

        for acc in accs:
            pltpu.matmul_pop(acc)
        for slot in range(min(2, total)):
            push(slot)
        for slot in range(total):
            if slot + 2 < total:
                push(slot + 2)
            if slot in copies:
                copies[slot].wait()
            ref, at = places[slot] if slot < ready else (buf_ref, slot - ready)
            both = [ref[at, part] for part in range(2)]
            left = jnp.concatenate(both, axis=1)
            if left.shape[0] % 16:
                left = jnp.concatenate([left, left[:8]], axis=0)
            pltpu.matmul_acc_lhs(accs[slot % 2], left, load_staged_rhs=slot // 2 % 2)
            if (slot + 1) % group == 0 or slot + 1 == total:
                g = slot // group
                value = pltpu.matmul_pop(acc_even) + pltpu.matmul_pop(acc_odd)
                for f in range(freq):
                    rows = value[f * plan.block : (f + 1) * plan.block]
                    at = (f * (last_group - first_group) + g) * plan.block_pad
                    own_ref[at : at + plan.block] = rows[:, :LANES]
                    other_ref[at : at + plan.block] = rows[:, LANES:]

    shape = (up(plan.sensors, 16), 2 * LANES)
    pl.run_scoped(multiply, pltpu.ACC(0)(shape, F32), pltpu.ACC(1)(shape, F32))
    for copy in late:
        copy.wait()


def join_kernel(plan, sizes, last, *refs):
    pairs, outs = refs[: 2 * len(sizes)], refs[2 * len(sizes) :]
    me, pad, fold_rows = lax.axis_index("freq"), plan.block_pad, plan.fold_rows
    lane = lax.broadcasted_iota(I32, (fold_rows, LANES), 1) % plan.group
    whole_groups = sum(sizes) - last
    for k in range(plan.freq):
        done = 0
        for call_at, size in enumerate(sizes):
            own_ref, other_ref = pairs[2 * call_at : 2 * call_at + 2]
            at = pl.multiple_of((me ^ k) * (size * pad), 8)
            value = own_ref[pl.ds(at, size * pad)] + other_ref[pl.ds(at, size * pad)]
            full = min(size, whole_groups - done) * pad
            if full:
                outs[k][done * pad : done * pad + full] = value[:full].astype(BF16)
            done += size
        if not last:
            continue
        tile, packed = value[full:], jnp.zeros((fold_rows, LANES), F32)
        for j in range(plan.fold):
            part = tile[j * fold_rows : (j + 1) * fold_rows]
            if part.shape[0] < fold_rows:
                rest = jnp.zeros((fold_rows - part.shape[0], LANES), F32)
                part = jnp.concatenate([part, rest], axis=0)
            if j:
                part = pltpu.roll(part, j * plan.last, 1)
            packed = jnp.where(lane // plan.last == j, part, packed)
        outs[k][whole_groups * pad :] = packed.astype(BF16)


def inverse_kernel(plan, hits_ref, high_ref, low_ref, *rest):
    freq, group, pad = plan.freq, plan.group, plan.block_pad
    early, late, rest = by_step(rest[:freq]), by_step(rest[freq : 2 * freq]), rest[2 * freq :]
    outs, (joined_ref,) = rest[: plan.pieces], rest[plan.pieces :]
    me, piece = lax.axis_index("freq"), lax.axis_index("param") // 2
    lane = lax.broadcasted_iota(I32, (pad, LANES), 1)
    real_row = lax.broadcasted_iota(I32, (pad, LANES), 0) < plan.block
    for k in range(freq):
        tiles = [early[k][at : at + pad].astype(F32) for at in range(0, early[k].shape[0], pad)]
        whole_rows = late[k].shape[0] - plan.fold_rows
        tiles += [late[k][at : at + pad].astype(F32) for at in range(0, whole_rows, pad)]
        packed = late[k][whole_rows:].astype(F32)
        folds = [packed] + [
            pltpu.roll(packed, LANES - j * plan.last, 1) for j in range(1, plan.fold)
        ]
        tiles.append(jnp.concatenate(folds, axis=0)[:pad])
        for comp in range(plan.comps):
            value = jnp.zeros((pad, LANES), F32)
            for g, tile in enumerate(tiles):
                inside = (lane // group == (g + comp) % plan.comps) & real_row
                value = jnp.where(inside, tile, value)
            if comp:
                value = pltpu.roll(value, LANES - comp * group, 1)
            at = comp * pad
            joined_ref[at : at + pad, k * LANES : (k + 1) * LANES] = value.astype(BF16)
    hits = jnp.concatenate([hits_ref[me ^ k] for k in range(freq)], axis=1)
    by_bin = dot_nt(joined_ref[...], hits)
    bins = lax.broadcasted_iota(I32, (1, plan.bins), 1)
    weight = jnp.where((bins == 0) | (bins == plan.steps), 1.0, 2.0)
    rows = []
    for c in range(plan.half):
        real = by_bin[2 * c * pad : (2 * c + 1) * pad] * weight
        imag = by_bin[(2 * c + 1) * pad : (2 * c + 2) * pad] * -weight
        rows.append(jnp.concatenate([real, imag], axis=1).astype(BF16))
    high = jnp.concatenate(rows, axis=0)
    scale = 1.0 / math.sqrt(2.0 * (plan.steps + 1))
    for k in range(plan.pieces):
        at = pl.multiple_of((piece ^ k) * plan.span_pad, plan.span_pad)
        table_high = high_ref[pl.ds(at, plan.span_pad), :]
        table_low = low_ref[pl.ds(at, plan.span_pad), :]
        value = (dot_nt(high, table_high) + dot_nt(high, table_low)) * scale
        outs[k][...] = pack(plan, value).astype(outs[k].dtype)


def stack_kernel(*refs):
    size = refs[0].shape[0]
    for k, ref in enumerate(refs[:-1]):
        refs[-1][k * size : (k + 1) * size] = ref[...]


def sum_kernel(*refs):
    value = refs[0][...]
    for ref in refs[1:-1]:
        value = value + ref[...].astype(F32)
    refs[-1][...] = value.astype(BF16)


def output_kernel(plan, *refs):
    out_ref = refs[-1]
    piece, core = lax.axis_index("param") // 2, lax.axis_index("param") % 2
    width = plan.span_pad
    time = lax.broadcasted_iota(I32, (plan.steps, plan.pieces * width), 0)
    lane = lax.broadcasted_iota(I32, (plan.steps, plan.pieces * width), 1)
    inside = lane % width
    target = (lane // width ^ piece) * plan.span + inside
    pick = jnp.where((time == target) & (inside < plan.span), 1.0, 0.0).astype(BF16)
    for side in range(2):
        parts = [
            unpack(plan, refs[side][k * plan.base : (k + 1) * plan.base].astype(F32)).astype(BF16)
            for k in range(plan.pieces)
        ]
        value = dot_nt(jnp.concatenate(parts, axis=1), pick)
        for c in range(plan.half):
            at = c * plan.block_pad
            out_ref[:, (core ^ side) * plan.half + c, :] = value[at : at + plan.block]


def cost(flops, moved):
    return pl.CostEstimate(flops=flops, bytes_accessed=moved, transcendentals=0)


def call(body, out_shapes, args, in_specs=None, scratch=(), cost=None, limit=LIMIT):
    whole = pl.BlockSpec(memory_space=VMEM)
    return pl.pallas_call(
        body,
        out_shape=out_shapes,
        in_specs=in_specs or [whole] * len(args),
        out_specs=jax.tree.map(lambda _: whole, out_shapes),
        scratch_shapes=list(scratch),
        cost_estimate=cost,
        compiler_params=pltpu.CompilerParams(vmem_limit_bytes=limit),
    )(*args)


def shards(mesh, sources, kernel, bin_of_slot):
    plan = Plan(mesh, sources, kernel, bin_of_slot)
    freq, pieces = plan.freq, plan.pieces
    shape = jax.ShapeDtypeStruct
    high, low = plan.tables()
    bins = bin_of_slot.reshape(1, plan.slots)
    row = VMEM((8, plan.slots_pad), I32)
    whole = pl.BlockSpec(memory_space=VMEM)

    def over_freq(values):
        moved = {
            k: lax.ppermute(values[k], "freq", [(i, i ^ k) for i in range(freq)])
            for k in range(freq - 1, 0, -1)
        }
        return [values[0], *moved.values()]

    def to_piece(value, k):
        pairs = [(2 * z + h, 2 * (z ^ k) + h) for z in range(pieces) for h in range(2)]
        return lax.ppermute(value, "param", pairs)

    def to_core(value):
        return lax.ppermute(value, "param", [(i, i ^ 1) for i in range(plan.param)])

    ends = [g for g in (plan.groups - 2, plan.groups - 1, plan.groups) if g > 0]
    ranges = list(zip([0, *ends], ends))
    sizes = [end - begin for begin, end in ranges]
    totals = [min(end * plan.group, plan.here) - begin * plan.group for begin, end in ranges]
    block = (2, plan.sensors, plan.depth)
    early = min(totals[0] // CHUNK, EARLY) * CHUNK

    spectra = call(
        functools.partial(forward_kernel, plan),
        [shape((2 * plan.count, plan.mine, LANES), BF16)] * freq,
        (bins, jnp.transpose(sources, (0, 2, 1)), high, low),
        in_specs=[pl.BlockSpec(memory_space=pltpu.HBM)] * 4,
        scratch=[
            VMEM(bins.shape, I32),
            VMEM((plan.count, plan.mine, plan.steps), F32),
            VMEM(high.shape, BF16),
            VMEM(low.shape, BF16),
            row,
            VMEM((plan.count * plan.mine, pieces * plan.span_pad), F32),
            VMEM((freq, 2 * plan.count, plan.mine, LANES), BF16),
            pltpu.SemaphoreType.DMA((4,)),
        ],
        cost=cost(2 * 10**9, 2 * high.size),
        limit=FULL - ROOM,
    )
    arrived = over_freq(spectra)

    hbm = pl.BlockSpec(memory_space=pltpu.HBM)
    ready, hits = call(
        functools.partial(load_kernel, plan, early),
        [shape((early, *block), BF16), shape((freq, plan.bins, LANES), BF16)],
        (spectra[0], bins, kernel),
        in_specs=[pl.BlockSpec(memory_space=pl.ANY), whole, hbm],
        scratch=[row, pltpu.SemaphoreType.DMA((-(-early // CHUNK),))],
        cost=cost(4 * 10**9, 4 * early * plan.sensors * plan.depth),
    )
    ready = [ready]
    def join(at, last):
        groups = [sizes[i] for i in at]
        rows = (sum(groups) - last) * plan.block_pad + last * plan.fold_rows
        return call(
            functools.partial(join_kernel, plan, groups, last),
            [shape((rows, LANES), BF16)] * freq,
            [array for i in at for array in pairs[2 * i : 2 * i + 2]],
        )

    pairs = []
    for index, (begin, end) in enumerate(ranges):
        total, held = totals[index], [array.shape[0] for array in ready]
        rest = total - sum(held)
        ahead = min(totals[index + 1], AHEAD * CHUNK) if index + 1 < len(totals) else 0
        streams = int(rest > 0 or ahead > 0)
        size = shape((freq * sizes[index] * plan.block_pad, LANES), F32)
        own, other, *later = call(
            functools.partial(response_kernel, plan, begin, end, held, ahead),
            [size, size] + ([shape((ahead, *block), BF16)] if ahead else []),
            (*arrived, *ready) + (kernel,) * streams,
            in_specs=[whole] * (freq + len(ready)) + [hbm] * streams,
            scratch=[
                VMEM((max(rest, CHUNK), *block), BF16),
                VMEM((2 * plan.count, plan.depth, LANES), BF16),
                VMEM((end - begin, 2 * plan.depth, 2 * LANES), BF16),
                pltpu.SemaphoreType.DMA((-(-rest // CHUNK) + -(-ahead // CHUNK) + 1,)),
            ],
            cost=cost(total * 512 * plan.sensors * plan.depth, 4 * total * plan.sensors * plan.depth),
        )
        ready = later
        pairs += [own, to_core(other)]
        if index == len(ranges) - 2:
            joined, ready = lax.optimization_barrier((join([0], 0), ready))
            parts = over_freq(joined)
    parts += over_freq(join(list(range(1, len(sizes))), 1))

    partial = call(
        functools.partial(inverse_kernel, plan),
        [shape((plan.base, plan.span_pad), BF16 if k else F32) for k in range(pieces)],
        (hits, high, low, *parts),
        scratch=[
            VMEM((plan.comps * plan.block_pad, freq * LANES), BF16),
        ],
    )
    received = [to_piece(partial[k], k) for k in range(pieces - 1, 0, -1)]
    piece = call(sum_kernel, shape((plan.base, plan.span_pad), BF16), (partial[0], *received))
    mine = [piece] + [to_piece(piece, k) for k in range(1, pieces)]
    mine = call(stack_kernel, shape((pieces * plan.base, plan.span_pad), BF16), mine)
    theirs = to_core(mine)
    by_sensor = call(
        functools.partial(output_kernel, plan),
        shape((plan.block, plan.count, plan.steps), F32),
        (mine, theirs),
    )
    return jnp.transpose(by_sensor, (1, 2, 0))


def solution(mesh):
    return jax.shard_map(
        functools.partial(shards, mesh),
        mesh=mesh,
        in_specs=(P(None, None, ("param", "freq")), P("freq", None, None, "param"), P()),
        out_specs=P(None, None, "freq"),
        check_vma=False,
    )
```

```python
import functools
import math

import jax
import jax.numpy as jnp
import numpy as np
from jax import lax
from jax.experimental import pallas as pl
from jax.experimental.pallas import tpu as pltpu
from jax.sharding import PartitionSpec as P

LANES = 128
BF16, F32, I32 = jnp.bfloat16, jnp.float32, jnp.int32
VMEM = pltpu.VMEM
MIB = 1024 * 1024
LIMIT = 16 * MIB
FULL = 67043328
ROOM = 10 * MIB + 400 * 1024
CHUNK, EARLY, AHEAD = 8, 5, 2


def up(value, unit):
    return -(-value // unit) * unit


def by_step(refs):
    return [refs[0], *refs[:0:-1]]


def dot_nt(left, right):
    return lax.dot_general(left, right, (((1,), (1,)), ((), ())), preferred_element_type=F32)


def dot_nn(left, right):
    return jnp.dot(left, right, preferred_element_type=F32)


def halves(value):
    high = value.astype(BF16)
    return high, (value - high.astype(F32)).astype(BF16)


class Plan:
    def __init__(self, mesh, sources, kernel, bin_of_slot):
        self.freq = mesh.shape["freq"]
        self.param = mesh.shape["param"]
        self.pieces = self.param // 2
        self.count, self.steps, self.mine = sources.shape
        self.slots = bin_of_slot.shape[0]
        self.here, _, self.sensors, self.depth = kernel.shape
        self.half = self.count // 2
        self.comps = 2 * self.half
        self.group = LANES // self.comps
        self.groups = -(-self.here // self.group)
        self.block = self.sensors // self.freq
        self.block_pad = up(self.block, 8)
        self.bins = up(self.steps + 1, LANES)
        self.span = -(-self.steps // self.pieces)
        self.span_pad = up(self.span, LANES)
        self.slots_pad = up(self.slots, LANES)
        self.last = self.here - (self.groups - 1) * self.group
        self.fold = self.group // self.last
        self.fold_rows = up(-(-self.block_pad // self.fold), 8)
        self.rows = self.half * self.block_pad
        self.spare = self.span_pad - self.span
        self.base = self.rows
        if self.spare:
            self.cuts = -(-self.span // self.spare)
            while (self.rows - self.base + 16) * self.cuts <= self.base - 16:
                self.base -= 16
        self.tail = self.rows - self.base
        assert self.here <= LANES and self.depth == self.mine * self.freq
        assert self.freq & (self.freq - 1) == 0 and self.pieces & (self.pieces - 1) == 0

    def tables(self):
        times = np.arange(self.steps)
        rows = times // self.span * self.span_pad + times % self.span
        bins = np.arange(self.steps + 1)
        angle = (times[:, None] * bins[None, :] % (2 * self.steps)) * (math.pi / self.steps)
        table = np.zeros((self.pieces * self.span_pad, 2 * self.bins), np.float64)
        table[rows, : self.steps + 1] = np.cos(angle)
        table[rows, self.bins : self.bins + self.steps + 1] = np.sin(angle)
        high = table.astype(jnp.bfloat16)
        low = (table - high.astype(np.float64)).astype(jnp.bfloat16)
        return high, low


def pack(plan, value):
    if not plan.tail:
        return value
    tail, parts = value[plan.base :], []
    for j in range(plan.cuts):
        parts.append(pltpu.roll(tail, (plan.span - plan.spare * j) % plan.span_pad, 1))
    left = plan.base - plan.tail * plan.cuts
    if left:
        parts.append(jnp.zeros((left, plan.span_pad), F32))
    lane = lax.broadcasted_iota(I32, (plan.base, plan.span_pad), 1)
    return jnp.where(lane < plan.span, value[: plan.base], jnp.concatenate(parts, axis=0))


def unpack(plan, value):
    if not plan.tail:
        return value
    tail = jnp.zeros((plan.tail, plan.span_pad), F32)
    lane = lax.broadcasted_iota(I32, tail.shape, 1)
    for j in range(plan.cuts):
        part = value[plan.tail * j : plan.tail * (j + 1)]
        part = pltpu.roll(part, (plan.spare * j - plan.span) % plan.span_pad, 1)
        tail = jnp.where(lane // plan.spare == j, part, tail)
    return jnp.concatenate([value, tail], axis=0)


def bin_row(plan, bins_ref, row_ref):
    row_ref[...] = jnp.full(row_ref.shape, -1, I32)
    row_ref[0:1, 0 : plan.slots] = bins_ref[...]
    return row_ref[0:1, :]


def slot_hits(plan, row, shard):
    shift = (-plan.here * shard) % plan.slots_pad
    if shift:
        row = pltpu.roll(row, shift, 1)
    row = row[:, :LANES]
    lane = lax.broadcasted_iota(I32, (1, LANES), 1)
    row = jnp.where(lane < plan.here, row, -1)
    bins = lax.broadcasted_iota(I32, (plan.bins, LANES), 0)
    return jnp.where(bins == row, 1.0, 0.0).astype(BF16)


def stream(kern_ref, first, size, target, sem_ref, index):
    return pltpu.make_async_copy(
        kern_ref.at[pl.ds(first, size)], target.at[pl.ds(0, size)], sem_ref.at[index]
    )


def forward_kernel(plan, *refs):
    ins, outs, rest = refs[:4], refs[4 : 4 + plan.freq], refs[4 + plan.freq :]
    bins_ref, src_ref, high_ref, low_ref, row_ref, time_ref, send_ref, sem_ref = rest
    copies = [
        pltpu.make_async_copy(source, target, sem_ref.at[i])
        for i, (source, target) in enumerate(zip(ins, rest))
    ]
    for copy in copies:
        copy.start()
    for copy in copies:
        copy.wait()
    me = lax.axis_index("freq")
    time_ref[...] = jnp.zeros(time_ref.shape, F32)
    rows = plan.count * plan.mine
    for z in range(plan.pieces):
        first = z * plan.span
        size = min(plan.span, plan.steps - first)
        at = z * plan.span_pad
        time_ref[:, at : at + size] = src_ref[:, :, first : first + size].reshape(rows, size)
    high, low = halves(time_ref[...])
    spectrum = (
        dot_nn(high, high_ref[...]) + dot_nn(high, low_ref[...]) + dot_nn(low, high_ref[...])
    )
    scale = 1.0 / math.sqrt(plan.steps)
    both = jnp.concatenate(
        [
            (spectrum[:, : plan.bins] * scale).astype(BF16),
            (spectrum[:, plan.bins :] * -scale).astype(BF16),
        ],
        axis=0,
    )
    row = bin_row(plan, bins_ref, row_ref)
    for shard in range(plan.freq):
        picked = dot_nn(both, slot_hits(plan, row, shard))
        for c in range(plan.count):
            for part in range(2):
                first = part * rows + c * plan.mine
                comp = 2 * (c % plan.half) + part
                value = picked[first : first + plan.mine]
                if comp:
                    value = pltpu.roll(value, comp * plan.group, 1)
                send_ref[shard, 2 * c + part] = value.astype(BF16)
    for k in range(plan.freq):
        outs[k][...] = send_ref[me ^ k]


def load_kernel(plan, count, after_ref, bins_ref, kern_ref, out_ref, hits_ref, row_ref, sem_ref):
    starts = range(0, count, CHUNK)
    copies = [
        stream(kern_ref, at, min(CHUNK, count - at), out_ref.at[pl.ds(at, CHUNK)], sem_ref, i)
        for i, at in enumerate(starts)
    ]
    for copy in copies:
        copy.start()
    row = bin_row(plan, bins_ref, row_ref)
    for shard in range(plan.freq):
        hits_ref[shard] = slot_hits(plan, row, shard)
    for copy in copies:
        copy.wait()


def response_kernel(plan, begin, end, held, ahead, *refs):
    freq, group = plan.freq, plan.group
    arrived, refs = by_step(refs[:freq]), refs[freq:]
    held_refs, refs = refs[: len(held)], refs[len(held) :]
    if ahead or sum(held) < min(end * group, plan.here) - begin * group:
        kern_ref, refs = refs[0], refs[1:]
    places = [(ref, at) for ref, size in zip(held_refs, held) for at in range(size)]
    ready = len(places)
    own_ref, other_ref, refs = refs[0], refs[1], refs[2:]
    if ahead:
        ahead_ref, refs = refs[0], refs[1:]
    buf_ref, spec_ref, rhs_ref, sem_ref = refs
    first_group, last_group = begin, end
    first = first_group * group
    total = min(last_group * group, plan.here) - first
    copies, late = {}, []
    for at in range(ready, total, CHUNK):
        size = min(CHUNK, total - at)
        target = buf_ref.at[pl.ds(at - ready, size)]
        copies[at] = stream(kern_ref, first + at, size, target, sem_ref, len(copies))
    for at in range(0, ahead, CHUNK):
        size = min(CHUNK, ahead - at)
        target = ahead_ref.at[pl.ds(at, size)]
        index = len(copies) + len(late)
        late.append(stream(kern_ref, first + total + at, size, target, sem_ref, index))
    for copy in [*copies.values(), *late]:
        copy.start()
    me, core = lax.axis_index("freq"), lax.axis_index("param") % 2
    for k in range(freq):
        at = pl.multiple_of((me ^ k) * plan.mine, plan.mine)
        spec_ref[:, pl.ds(at, plan.mine), :] = arrived[k][...]
    lane = lax.broadcasted_iota(I32, (plan.depth, LANES), 1)
    for g in range(first_group, last_group):
        for side in range(2):
            base = (core ^ side) * plan.comps
            place = (lane // group - g) % plan.comps
            real = spec_ref[base].astype(F32)
            for comp in range(1, plan.comps):
                real = jnp.where(place == comp, spec_ref[base + comp].astype(F32), real)
            imag = jnp.where(
                place % 2 == 0, -pltpu.roll(real, LANES - group, 1), pltpu.roll(real, group, 1)
            )
            cols = slice(side * LANES, (side + 1) * LANES)
            rhs_ref[g - first_group, : plan.depth, cols] = real.astype(BF16)
            rhs_ref[g - first_group, plan.depth :, cols] = imag.astype(BF16)
    within = lax.broadcasted_iota(I32, (2 * plan.depth, 2 * LANES), 1) % group

    def multiply(acc_even, acc_odd):
        accs = (acc_even, acc_odd)

        def push(slot):
            weights = rhs_ref[slot // group]
            pltpu.matmul_push_rhs(
                jnp.where(within == slot % group, weights, jnp.zeros_like(weights)),
                staging_register=slot // 2 % 2,
                mxu_index=slot % 2,
            )

        for acc in accs:
            pltpu.matmul_pop(acc)
        for slot in range(min(2, total)):
            push(slot)
        for slot in range(total):
            if slot + 2 < total:
                push(slot + 2)
            if slot in copies:
                copies[slot].wait()
            ref, at = places[slot] if slot < ready else (buf_ref, slot - ready)
            both = [ref[at, part] for part in range(2)]
            left = jnp.concatenate(both, axis=1)
            if left.shape[0] % 16:
                left = jnp.concatenate([left, left[:8]], axis=0)
            pltpu.matmul_acc_lhs(accs[slot % 2], left, load_staged_rhs=slot // 2 % 2)
            if (slot + 1) % group == 0 or slot + 1 == total:
                g = slot // group
                value = pltpu.matmul_pop(acc_even) + pltpu.matmul_pop(acc_odd)
                for f in range(freq):
                    rows = value[f * plan.block : (f + 1) * plan.block]
                    at = (f * (last_group - first_group) + g) * plan.block_pad
                    own_ref[at : at + plan.block] = rows[:, :LANES]
                    other_ref[at : at + plan.block] = rows[:, LANES:]

    shape = (up(plan.sensors, 16), 2 * LANES)
    pl.run_scoped(multiply, pltpu.ACC(0)(shape, F32), pltpu.ACC(1)(shape, F32))
    for copy in late:
        copy.wait()


def join_kernel(plan, sizes, last, *refs):
    pairs, outs = refs[: 2 * len(sizes)], refs[2 * len(sizes) :]
    me, pad, fold_rows = lax.axis_index("freq"), plan.block_pad, plan.fold_rows
    lane = lax.broadcasted_iota(I32, (fold_rows, LANES), 1) % plan.group
    whole_groups = sum(sizes) - last
    for k in range(plan.freq):
        done = 0
        for call_at, size in enumerate(sizes):
            own_ref, other_ref = pairs[2 * call_at : 2 * call_at + 2]
            at = pl.multiple_of((me ^ k) * (size * pad), 8)
            value = own_ref[pl.ds(at, size * pad)] + other_ref[pl.ds(at, size * pad)]
            full = min(size, whole_groups - done) * pad
            if full:
                outs[k][done * pad : done * pad + full] = value[:full].astype(BF16)
            done += size
        if not last:
            continue
        tile, packed = value[full:], jnp.zeros((fold_rows, LANES), F32)
        for j in range(plan.fold):
            part = tile[j * fold_rows : (j + 1) * fold_rows]
            if part.shape[0] < fold_rows:
                rest = jnp.zeros((fold_rows - part.shape[0], LANES), F32)
                part = jnp.concatenate([part, rest], axis=0)
            if j:
                part = pltpu.roll(part, j * plan.last, 1)
            packed = jnp.where(lane // plan.last == j, part, packed)
        outs[k][whole_groups * pad :] = packed.astype(BF16)


def inverse_kernel(plan, hits_ref, high_ref, low_ref, *rest):
    freq, group, pad = plan.freq, plan.group, plan.block_pad
    early, late, rest = by_step(rest[:freq]), by_step(rest[freq : 2 * freq]), rest[2 * freq :]
    outs, (joined_ref,) = rest[: plan.pieces], rest[plan.pieces :]
    me, piece = lax.axis_index("freq"), lax.axis_index("param") // 2
    lane = lax.broadcasted_iota(I32, (pad, LANES), 1)
    real_row = lax.broadcasted_iota(I32, (pad, LANES), 0) < plan.block
    for k in range(freq):
        tiles = [early[k][at : at + pad].astype(F32) for at in range(0, early[k].shape[0], pad)]
        whole_rows = late[k].shape[0] - plan.fold_rows
        tiles += [late[k][at : at + pad].astype(F32) for at in range(0, whole_rows, pad)]
        packed = late[k][whole_rows:].astype(F32)
        folds = [packed] + [
            pltpu.roll(packed, LANES - j * plan.last, 1) for j in range(1, plan.fold)
        ]
        tiles.append(jnp.concatenate(folds, axis=0)[:pad])
        for comp in range(plan.comps):
            value = jnp.zeros((pad, LANES), F32)
            for g, tile in enumerate(tiles):
                inside = (lane // group == (g + comp) % plan.comps) & real_row
                value = jnp.where(inside, tile, value)
            if comp:
                value = pltpu.roll(value, LANES - comp * group, 1)
            at = comp * pad
            joined_ref[at : at + pad, k * LANES : (k + 1) * LANES] = value.astype(BF16)
    hits = jnp.concatenate([hits_ref[me ^ k] for k in range(freq)], axis=1)
    by_bin = dot_nt(joined_ref[...], hits)
    bins = lax.broadcasted_iota(I32, (1, plan.bins), 1)
    weight = jnp.where((bins == 0) | (bins == plan.steps), 1.0, 2.0)
    rows = []
    for c in range(plan.half):
        real = by_bin[2 * c * pad : (2 * c + 1) * pad] * weight
        imag = by_bin[(2 * c + 1) * pad : (2 * c + 2) * pad] * -weight
        rows.append(jnp.concatenate([real, imag], axis=1).astype(BF16))
    high = jnp.concatenate(rows, axis=0)
    scale = 1.0 / math.sqrt(2.0 * (plan.steps + 1))
    for pair in range(0, plan.pieces, 2):
        at = [pl.multiple_of((piece ^ k) * plan.span_pad, plan.span_pad) for k in (pair, pair + 1)]
        tables = [
            jnp.concatenate([ref[pl.ds(i, plan.span_pad), :] for i in at], axis=0)
            for ref in (high_ref, low_ref)
        ]
        value = (dot_nt(high, tables[0]) + dot_nt(high, tables[1])) * scale
        for i in range(2):
            half = value[:, i * plan.span_pad : (i + 1) * plan.span_pad]
            outs[pair + i][...] = pack(plan, half).astype(outs[pair + i].dtype)


def stack_kernel(*refs):
    size = refs[0].shape[0]
    for k, ref in enumerate(refs[:-1]):
        refs[-1][k * size : (k + 1) * size] = ref[...]


def sum_kernel(*refs):
    value = refs[0][...]
    for ref in refs[1:-1]:
        value = value + ref[...].astype(F32)
    refs[-1][...] = value.astype(BF16)


def by_time(plan, ref, pick):
    parts = [
        unpack(plan, ref[k * plan.base : (k + 1) * plan.base].astype(F32)).astype(BF16)
        for k in range(plan.pieces)
    ]
    return dot_nt(jnp.concatenate(parts, axis=1), pick)


def time_kernel(plan, ref, out_ref, pick_ref):
    piece, width = lax.axis_index("param") // 2, plan.span_pad
    time = lax.broadcasted_iota(I32, (plan.steps, plan.pieces * width), 0)
    lane = lax.broadcasted_iota(I32, (plan.steps, plan.pieces * width), 1)
    inside = lane % width
    target = (lane // width ^ piece) * plan.span + inside
    pick = jnp.where((time == target) & (inside < plan.span), 1.0, 0.0).astype(BF16)
    pick_ref[...] = pick
    out_ref[...] = by_time(plan, ref, pick)


def output_kernel(plan, mine_ref, theirs_ref, pick_ref, out_ref):
    core = lax.axis_index("param") % 2
    for side in range(2):
        value = by_time(plan, theirs_ref, pick_ref[...]) if side else mine_ref[...]
        for c in range(plan.half):
            at = c * plan.block_pad
            out_ref[:, (core ^ side) * plan.half + c, :] = value[at : at + plan.block]


def cost(flops, moved):
    return pl.CostEstimate(flops=flops, bytes_accessed=moved, transcendentals=0)


def call(body, out_shapes, args, in_specs=None, scratch=(), cost=None, limit=LIMIT):
    whole = pl.BlockSpec(memory_space=VMEM)
    return pl.pallas_call(
        body,
        out_shape=out_shapes,
        in_specs=in_specs or [whole] * len(args),
        out_specs=jax.tree.map(lambda _: whole, out_shapes),
        scratch_shapes=list(scratch),
        cost_estimate=cost,
        compiler_params=pltpu.CompilerParams(vmem_limit_bytes=limit),
    )(*args)


def shards(mesh, sources, kernel, bin_of_slot):
    plan = Plan(mesh, sources, kernel, bin_of_slot)
    freq, pieces = plan.freq, plan.pieces
    shape = jax.ShapeDtypeStruct
    high, low = plan.tables()
    bins = bin_of_slot.reshape(1, plan.slots)
    row = VMEM((8, plan.slots_pad), I32)
    whole = pl.BlockSpec(memory_space=VMEM)

    def over_freq(values):
        moved = {
            k: lax.ppermute(values[k], "freq", [(i, i ^ k) for i in range(freq)])
            for k in range(freq - 1, 0, -1)
        }
        return [values[0], *moved.values()]

    def to_piece(value, k):
        pairs = [(2 * z + h, 2 * (z ^ k) + h) for z in range(pieces) for h in range(2)]
        return lax.ppermute(value, "param", pairs)

    def to_core(value):
        return lax.ppermute(value, "param", [(i, i ^ 1) for i in range(plan.param)])

    ends = [g for g in (plan.groups - 2, plan.groups - 1, plan.groups) if g > 0]
    ranges = list(zip([0, *ends], ends))
    sizes = [end - begin for begin, end in ranges]
    totals = [min(end * plan.group, plan.here) - begin * plan.group for begin, end in ranges]
    block = (2, plan.sensors, plan.depth)
    early = min(totals[0] // CHUNK, EARLY) * CHUNK

    spectra = call(
        functools.partial(forward_kernel, plan),
        [shape((2 * plan.count, plan.mine, LANES), BF16)] * freq,
        (bins, jnp.transpose(sources, (0, 2, 1)), high, low),
        in_specs=[pl.BlockSpec(memory_space=pltpu.HBM)] * 4,
        scratch=[
            VMEM(bins.shape, I32),
            VMEM((plan.count, plan.mine, plan.steps), F32),
            VMEM(high.shape, BF16),
            VMEM(low.shape, BF16),
            row,
            VMEM((plan.count * plan.mine, pieces * plan.span_pad), F32),
            VMEM((freq, 2 * plan.count, plan.mine, LANES), BF16),
            pltpu.SemaphoreType.DMA((4,)),
        ],
        cost=cost(2 * 10**9, 2 * high.size),
        limit=FULL - ROOM,
    )
    arrived = over_freq(spectra)

    hbm = pl.BlockSpec(memory_space=pltpu.HBM)
    ready, hits = call(
        functools.partial(load_kernel, plan, early),
        [shape((early, *block), BF16), shape((freq, plan.bins, LANES), BF16)],
        (spectra[0], bins, kernel),
        in_specs=[pl.BlockSpec(memory_space=pl.ANY), whole, hbm],
        scratch=[row, pltpu.SemaphoreType.DMA((-(-early // CHUNK),))],
        cost=cost(4 * 10**9, 4 * early * plan.sensors * plan.depth),
    )
    ready = [ready]
    def join(at, last):
        groups = [sizes[i] for i in at]
        rows = (sum(groups) - last) * plan.block_pad + last * plan.fold_rows
        return call(
            functools.partial(join_kernel, plan, groups, last),
            [shape((rows, LANES), BF16)] * freq,
            [array for i in at for array in pairs[2 * i : 2 * i + 2]],
        )

    pairs = []
    for index, (begin, end) in enumerate(ranges):
        total, held = totals[index], [array.shape[0] for array in ready]
        rest = total - sum(held)
        ahead = min(totals[index + 1], AHEAD * CHUNK) if index + 1 < len(totals) else 0
        streams = int(rest > 0 or ahead > 0)
        size = shape((freq * sizes[index] * plan.block_pad, LANES), F32)
        own, other, *later = call(
            functools.partial(response_kernel, plan, begin, end, held, ahead),
            [size, size] + ([shape((ahead, *block), BF16)] if ahead else []),
            (*arrived, *ready) + (kernel,) * streams,
            in_specs=[whole] * (freq + len(ready)) + [hbm] * streams,
            scratch=[
                VMEM((max(rest, CHUNK), *block), BF16),
                VMEM((2 * plan.count, plan.depth, LANES), BF16),
                VMEM((end - begin, 2 * plan.depth, 2 * LANES), BF16),
                pltpu.SemaphoreType.DMA((-(-rest // CHUNK) + -(-ahead // CHUNK) + 1,)),
            ],
            cost=cost(total * 512 * plan.sensors * plan.depth, 4 * total * plan.sensors * plan.depth),
        )
        ready = later
        pairs += [own, to_core(other)]
        if index == len(ranges) - 2:
            joined, ready = lax.optimization_barrier((join([0], 0), ready))
            parts = over_freq(joined)
    parts += over_freq(join(list(range(1, len(sizes))), 1))

    partial = call(
        functools.partial(inverse_kernel, plan),
        [shape((plan.base, plan.span_pad), BF16 if k else F32) for k in range(pieces)],
        (hits, high, low, *parts),
        scratch=[
            VMEM((plan.comps * plan.block_pad, freq * LANES), BF16),
        ],
    )
    received = [to_piece(partial[k], k) for k in range(pieces - 1, 0, -1)]
    piece = call(sum_kernel, shape((plan.base, plan.span_pad), BF16), (partial[0], *received))
    mine = [piece] + [to_piece(piece, k) for k in range(1, pieces)]
    mine = call(stack_kernel, shape((pieces * plan.base, plan.span_pad), BF16), mine)
    theirs = to_core(mine)
    ours, pick = call(
        functools.partial(time_kernel, plan),
        [
            shape((plan.rows, plan.steps), F32),
            shape((plan.steps, pieces * plan.span_pad), BF16),
        ],
        (mine,),
        cost=cost(10**9, 10**6),
    )
    by_sensor = call(
        functools.partial(output_kernel, plan),
        shape((plan.block, plan.count, plan.steps), F32),
        (ours, theirs, pick),
    )
    return jnp.transpose(by_sensor, (1, 2, 0))


def solution(mesh):
    return jax.shard_map(
        functools.partial(shards, mesh),
        mesh=mesh,
        in_specs=(P(None, None, ("param", "freq")), P("freq", None, None, "param"), P()),
        out_specs=P(None, None, "freq"),
        check_vma=False,
    )
```

```python
import functools
import math

import jax
import jax.numpy as jnp
import numpy as np
from jax import lax
from jax.experimental import pallas as pl
from jax.experimental.pallas import tpu as pltpu
from jax.sharding import PartitionSpec as P

LANES = 128
BF16, F32, I32 = jnp.bfloat16, jnp.float32, jnp.int32
VMEM = pltpu.VMEM
MIB = 1024 * 1024
LIMIT = 16 * MIB
FULL = 67043328
ROOM = 10 * MIB + 400 * 1024
CHUNK, EARLY, AHEAD = 8, 5, 2


def up(value, unit):
    return -(-value // unit) * unit


def by_step(refs):
    return [refs[0], *refs[:0:-1]]


def dot_nt(left, right):
    return lax.dot_general(left, right, (((1,), (1,)), ((), ())), preferred_element_type=F32)


def dot_nn(left, right):
    return jnp.dot(left, right, preferred_element_type=F32)


def halves(value):
    high = value.astype(BF16)
    return high, (value - high.astype(F32)).astype(BF16)


class Plan:
    def __init__(self, mesh, sources, kernel, bin_of_slot):
        self.freq = mesh.shape["freq"]
        self.param = mesh.shape["param"]
        self.pieces = self.param // 2
        self.count, self.steps, self.mine = sources.shape
        self.slots = bin_of_slot.shape[0]
        self.here, _, self.sensors, self.depth = kernel.shape
        self.half = self.count // 2
        self.comps = 2 * self.half
        self.group = LANES // self.comps
        self.groups = -(-self.here // self.group)
        self.block = self.sensors // self.freq
        self.block_pad = up(self.block, 8)
        self.bins = up(self.steps + 1, LANES)
        self.span = -(-self.steps // self.pieces)
        self.span_pad = up(self.span, LANES)
        self.slots_pad = up(self.slots, LANES)
        self.last = self.here - (self.groups - 1) * self.group
        self.fold = self.group // self.last
        self.fold_rows = up(-(-self.block_pad // self.fold), 8)
        self.rows = self.half * self.block_pad
        self.spare = self.span_pad - self.span
        self.base = self.rows
        if self.spare:
            self.cuts = -(-self.span // self.spare)
            while (self.rows - self.base + 16) * self.cuts <= self.base - 16:
                self.base -= 16
        self.tail = self.rows - self.base
        assert self.here <= LANES and self.depth == self.mine * self.freq
        assert self.freq & (self.freq - 1) == 0 and self.pieces & (self.pieces - 1) == 0

    def tables(self):
        times = np.arange(self.steps)
        rows = times // self.span * self.span_pad + times % self.span
        bins = np.arange(self.steps + 1)
        angle = (times[:, None] * bins[None, :] % (2 * self.steps)) * (math.pi / self.steps)
        table = np.zeros((self.pieces * self.span_pad, 2 * self.bins), np.float64)
        table[rows, : self.steps + 1] = np.cos(angle)
        table[rows, self.bins : self.bins + self.steps + 1] = np.sin(angle)
        high = table.astype(jnp.bfloat16)
        low = (table - high.astype(np.float64)).astype(jnp.bfloat16)
        return high, low


def pack(plan, value):
    if not plan.tail:
        return value
    tail, parts = value[plan.base :], []
    for j in range(plan.cuts):
        parts.append(pltpu.roll(tail, (plan.span - plan.spare * j) % plan.span_pad, 1))
    left = plan.base - plan.tail * plan.cuts
    if left:
        parts.append(jnp.zeros((left, plan.span_pad), F32))
    lane = lax.broadcasted_iota(I32, (plan.base, plan.span_pad), 1)
    return jnp.where(lane < plan.span, value[: plan.base], jnp.concatenate(parts, axis=0))


def unpack(plan, value):
    if not plan.tail:
        return value
    tail = jnp.zeros((plan.tail, plan.span_pad), F32)
    lane = lax.broadcasted_iota(I32, tail.shape, 1)
    for j in range(plan.cuts):
        part = value[plan.tail * j : plan.tail * (j + 1)]
        part = pltpu.roll(part, (plan.spare * j - plan.span) % plan.span_pad, 1)
        tail = jnp.where(lane // plan.spare == j, part, tail)
    return jnp.concatenate([value, tail], axis=0)


def bin_row(plan, bins_ref, row_ref):
    row_ref[...] = jnp.full(row_ref.shape, -1, I32)
    row_ref[0:1, 0 : plan.slots] = bins_ref[...]
    return row_ref[0:1, :]


def slot_hits(plan, row, shard):
    shift = (-plan.here * shard) % plan.slots_pad
    if shift:
        row = pltpu.roll(row, shift, 1)
    row = row[:, :LANES]
    lane = lax.broadcasted_iota(I32, (1, LANES), 1)
    row = jnp.where(lane < plan.here, row, -1)
    bins = lax.broadcasted_iota(I32, (plan.bins, LANES), 0)
    return jnp.where(bins == row, 1.0, 0.0).astype(BF16)


def stream(kern_ref, first, size, target, sem_ref, index):
    return pltpu.make_async_copy(
        kern_ref.at[pl.ds(first, size)], target.at[pl.ds(0, size)], sem_ref.at[index]
    )


def forward_kernel(plan, *refs):
    ins, outs, rest = refs[:4], refs[4 : 4 + plan.freq], refs[4 + plan.freq :]
    bins_ref, src_ref, high_ref, low_ref, row_ref, time_ref, send_ref, sem_ref = rest
    copies = [
        pltpu.make_async_copy(source, target, sem_ref.at[i])
        for i, (source, target) in enumerate(zip(ins, rest))
    ]
    for copy in copies:
        copy.start()
    for copy in copies:
        copy.wait()
    me = lax.axis_index("freq")
    time_ref[...] = jnp.zeros(time_ref.shape, F32)
    rows = plan.count * plan.mine
    for z in range(plan.pieces):
        first = z * plan.span
        size = min(plan.span, plan.steps - first)
        at = z * plan.span_pad
        time_ref[:, at : at + size] = src_ref[:, :, first : first + size].reshape(rows, size)
    high, low = halves(time_ref[...])
    spectrum = (
        dot_nn(high, high_ref[...]) + dot_nn(high, low_ref[...]) + dot_nn(low, high_ref[...])
    )
    scale = 1.0 / math.sqrt(plan.steps)
    both = jnp.concatenate(
        [
            (spectrum[:, : plan.bins] * scale).astype(BF16),
            (spectrum[:, plan.bins :] * -scale).astype(BF16),
        ],
        axis=0,
    )
    row = bin_row(plan, bins_ref, row_ref)
    for shard in range(plan.freq):
        picked = dot_nn(both, slot_hits(plan, row, shard))
        for c in range(plan.count):
            for part in range(2):
                first = part * rows + c * plan.mine
                comp = 2 * (c % plan.half) + part
                value = picked[first : first + plan.mine]
                if comp:
                    value = pltpu.roll(value, comp * plan.group, 1)
                send_ref[shard, 2 * c + part] = value.astype(BF16)
    for k in range(plan.freq):
        outs[k][...] = send_ref[me ^ k]


def load_kernel(plan, count, after_ref, bins_ref, kern_ref, out_ref, hits_ref, row_ref, sem_ref):
    starts = range(0, count, CHUNK)
    copies = [
        stream(kern_ref, at, min(CHUNK, count - at), out_ref.at[pl.ds(at, CHUNK)], sem_ref, i)
        for i, at in enumerate(starts)
    ]
    for copy in copies:
        copy.start()
    row = bin_row(plan, bins_ref, row_ref)
    for shard in range(plan.freq):
        hits_ref[shard] = slot_hits(plan, row, shard)
    for copy in copies:
        copy.wait()


def response_kernel(plan, begin, end, held, ahead, *refs):
    freq, group = plan.freq, plan.group
    arrived, refs = by_step(refs[:freq]), refs[freq:]
    held_refs, refs = refs[: len(held)], refs[len(held) :]
    if ahead or sum(held) < min(end * group, plan.here) - begin * group:
        kern_ref, refs = refs[0], refs[1:]
    places = [(ref, at) for ref, size in zip(held_refs, held) for at in range(size)]
    ready = len(places)
    own_ref, other_ref, refs = refs[0], refs[1], refs[2:]
    if ahead:
        ahead_ref, refs = refs[0], refs[1:]
    buf_ref, spec_ref, rhs_ref, sem_ref = refs
    first_group, last_group = begin, end
    first = first_group * group
    total = min(last_group * group, plan.here) - first
    copies, late = {}, []
    for at in range(ready, total, CHUNK):
        size = min(CHUNK, total - at)
        target = buf_ref.at[pl.ds(at - ready, size)]
        copies[at] = stream(kern_ref, first + at, size, target, sem_ref, len(copies))
    for at in range(0, ahead, CHUNK):
        size = min(CHUNK, ahead - at)
        target = ahead_ref.at[pl.ds(at, size)]
        index = len(copies) + len(late)
        late.append(stream(kern_ref, first + total + at, size, target, sem_ref, index))
    for copy in [*copies.values(), *late]:
        copy.start()
    me, core = lax.axis_index("freq"), lax.axis_index("param") % 2
    for k in range(freq):
        at = pl.multiple_of((me ^ k) * plan.mine, plan.mine)
        spec_ref[:, pl.ds(at, plan.mine), :] = arrived[k][...]
    lane = lax.broadcasted_iota(I32, (plan.depth, LANES), 1)
    for g in range(first_group, last_group):
        for side in range(2):
            base = (core ^ side) * plan.comps
            place = (lane // group - g) % plan.comps
            real = spec_ref[base].astype(F32)
            for comp in range(1, plan.comps):
                real = jnp.where(place == comp, spec_ref[base + comp].astype(F32), real)
            imag = jnp.where(
                place % 2 == 0, -pltpu.roll(real, LANES - group, 1), pltpu.roll(real, group, 1)
            )
            cols = slice(side * LANES, (side + 1) * LANES)
            rhs_ref[g - first_group, : plan.depth, cols] = real.astype(BF16)
            rhs_ref[g - first_group, plan.depth :, cols] = imag.astype(BF16)
    within = lax.broadcasted_iota(I32, (2 * plan.depth, 2 * LANES), 1) % group

    def multiply(acc_even, acc_odd):
        accs = (acc_even, acc_odd)

        def push(slot):
            weights = rhs_ref[slot // group]
            pltpu.matmul_push_rhs(
                jnp.where(within == slot % group, weights, jnp.zeros_like(weights)),
                staging_register=slot // 2 % 2,
                mxu_index=slot % 2,
            )

        for acc in accs:
            pltpu.matmul_pop(acc)
        for slot in range(min(2, total)):
            push(slot)
        for slot in range(total):
            if slot + 2 < total:
                push(slot + 2)
            if slot in copies:
                copies[slot].wait()
            ref, at = places[slot] if slot < ready else (buf_ref, slot - ready)
            both = [ref[at, part] for part in range(2)]
            left = jnp.concatenate(both, axis=1)
            if left.shape[0] % 16:
                left = jnp.concatenate([left, left[:8]], axis=0)
            pltpu.matmul_acc_lhs(accs[slot % 2], left, load_staged_rhs=slot // 2 % 2)
            if (slot + 1) % group == 0 or slot + 1 == total:
                g = slot // group
                value = pltpu.matmul_pop(acc_even) + pltpu.matmul_pop(acc_odd)
                for f in range(freq):
                    rows = value[f * plan.block : (f + 1) * plan.block]
                    at = (f * (last_group - first_group) + g) * plan.block_pad
                    own_ref[at : at + plan.block] = rows[:, :LANES]
                    other_ref[at : at + plan.block] = rows[:, LANES:]

    shape = (up(plan.sensors, 16), 2 * LANES)
    pl.run_scoped(multiply, pltpu.ACC(0)(shape, F32), pltpu.ACC(1)(shape, F32))
    for copy in late:
        copy.wait()


def join_kernel(plan, sizes, last, *refs):
    pairs, outs = refs[: 2 * len(sizes)], refs[2 * len(sizes) :]
    me, pad, fold_rows = lax.axis_index("freq"), plan.block_pad, plan.fold_rows
    lane = lax.broadcasted_iota(I32, (fold_rows, LANES), 1) % plan.group
    whole_groups = sum(sizes) - last
    for k in range(plan.freq):
        done = 0
        for call_at, size in enumerate(sizes):
            own_ref, other_ref = pairs[2 * call_at : 2 * call_at + 2]
            at = pl.multiple_of((me ^ k) * (size * pad), 8)
            value = own_ref[pl.ds(at, size * pad)] + other_ref[pl.ds(at, size * pad)]
            full = min(size, whole_groups - done) * pad
            if full:
                outs[k][done * pad : done * pad + full] = value[:full].astype(BF16)
            done += size
        if not last:
            continue
        tile, packed = value[full:], jnp.zeros((fold_rows, LANES), F32)
        for j in range(plan.fold):
            part = tile[j * fold_rows : (j + 1) * fold_rows]
            if part.shape[0] < fold_rows:
                rest = jnp.zeros((fold_rows - part.shape[0], LANES), F32)
                part = jnp.concatenate([part, rest], axis=0)
            if j:
                part = pltpu.roll(part, j * plan.last, 1)
            packed = jnp.where(lane // plan.last == j, part, packed)
        outs[k][whole_groups * pad :] = packed.astype(BF16)


def inverse_kernel(plan, hits_ref, high_ref, low_ref, *rest):
    freq, group, pad = plan.freq, plan.group, plan.block_pad
    early, late, rest = by_step(rest[:freq]), by_step(rest[freq : 2 * freq]), rest[2 * freq :]
    outs, (joined_ref,) = rest[: plan.pieces], rest[plan.pieces :]
    me, piece = lax.axis_index("freq"), lax.axis_index("param") // 2
    lane = lax.broadcasted_iota(I32, (pad, LANES), 1)
    real_row = lax.broadcasted_iota(I32, (pad, LANES), 0) < plan.block
    for k in range(freq):
        tiles = [early[k][at : at + pad].astype(F32) for at in range(0, early[k].shape[0], pad)]
        whole_rows = late[k].shape[0] - plan.fold_rows
        tiles += [late[k][at : at + pad].astype(F32) for at in range(0, whole_rows, pad)]
        packed = late[k][whole_rows:].astype(F32)
        folds = [packed] + [
            pltpu.roll(packed, LANES - j * plan.last, 1) for j in range(1, plan.fold)
        ]
        tiles.append(jnp.concatenate(folds, axis=0)[:pad])
        for comp in range(plan.comps):
            value = jnp.zeros((pad, LANES), F32)
            for g, tile in enumerate(tiles):
                inside = (lane // group == (g + comp) % plan.comps) & real_row
                if g == plan.groups - 1:
                    inside &= lane % group < plan.last
                value = jnp.where(inside, tile, value)
            if comp:
                value = pltpu.roll(value, LANES - comp * group, 1)
            at = comp * pad
            joined_ref[at : at + pad, k * LANES : (k + 1) * LANES] = value.astype(BF16)
    hits = jnp.concatenate([hits_ref[me ^ k] for k in range(freq)], axis=1)
    by_bin = dot_nt(joined_ref[...], hits)
    bins = lax.broadcasted_iota(I32, (1, plan.bins), 1)
    weight = jnp.where((bins == 0) | (bins == plan.steps), 1.0, 2.0)
    rows = []
    for c in range(plan.half):
        real = by_bin[2 * c * pad : (2 * c + 1) * pad] * weight
        imag = by_bin[(2 * c + 1) * pad : (2 * c + 2) * pad] * -weight
        rows.append(jnp.concatenate([real, imag], axis=1).astype(BF16))
    high = jnp.concatenate(rows, axis=0)
    scale = 1.0 / math.sqrt(2.0 * (plan.steps + 1))
    for pair in range(0, plan.pieces, 2):
        at = [pl.multiple_of((piece ^ k) * plan.span_pad, plan.span_pad) for k in (pair, pair + 1)]
        tables = [
            jnp.concatenate([ref[pl.ds(i, plan.span_pad), :] for i in at], axis=0)
            for ref in (high_ref, low_ref)
        ]
        value = (dot_nt(high, tables[0]) + dot_nt(high, tables[1])) * scale
        for i in range(2):
            half = value[:, i * plan.span_pad : (i + 1) * plan.span_pad]
            outs[pair + i][...] = pack(plan, half).astype(outs[pair + i].dtype)


def stack_kernel(*refs):
    size = refs[0].shape[0]
    for k, ref in enumerate(refs[:-1]):
        refs[-1][k * size : (k + 1) * size] = ref[...]


def sum_kernel(*refs):
    value = refs[0][...]
    for ref in refs[1:-1]:
        value = value + ref[...].astype(F32)
    refs[-1][...] = value.astype(BF16)


def by_time(plan, ref, pick):
    parts = [
        unpack(plan, ref[k * plan.base : (k + 1) * plan.base].astype(F32)).astype(BF16)
        for k in range(plan.pieces)
    ]
    return dot_nt(jnp.concatenate(parts, axis=1), pick)


def time_kernel(plan, ref, out_ref, pick_ref):
    piece, width = lax.axis_index("param") // 2, plan.span_pad
    time = lax.broadcasted_iota(I32, (plan.steps, plan.pieces * width), 0)
    lane = lax.broadcasted_iota(I32, (plan.steps, plan.pieces * width), 1)
    inside = lane % width
    target = (lane // width ^ piece) * plan.span + inside
    pick = jnp.where((time == target) & (inside < plan.span), 1.0, 0.0).astype(BF16)
    pick_ref[...] = pick
    out_ref[...] = by_time(plan, ref, pick)


def output_kernel(plan, mine_ref, theirs_ref, pick_ref, out_ref):
    core = lax.axis_index("param") % 2
    for side in range(2):
        value = by_time(plan, theirs_ref, pick_ref[...]) if side else mine_ref[...]
        for c in range(plan.half):
            at = c * plan.block_pad
            out_ref[:, (core ^ side) * plan.half + c, :] = value[at : at + plan.block]


def cost(flops, moved):
    return pl.CostEstimate(flops=flops, bytes_accessed=moved, transcendentals=0)


def call(body, out_shapes, args, in_specs=None, scratch=(), cost=None, limit=LIMIT):
    whole = pl.BlockSpec(memory_space=VMEM)
    return pl.pallas_call(
        body,
        out_shape=out_shapes,
        in_specs=in_specs or [whole] * len(args),
        out_specs=jax.tree.map(lambda _: whole, out_shapes),
        scratch_shapes=list(scratch),
        cost_estimate=cost,
        compiler_params=pltpu.CompilerParams(vmem_limit_bytes=limit),
    )(*args)


def shards(mesh, sources, kernel, bin_of_slot):
    plan = Plan(mesh, sources, kernel, bin_of_slot)
    freq, pieces = plan.freq, plan.pieces
    shape = jax.ShapeDtypeStruct
    high, low = plan.tables()
    bins = bin_of_slot.reshape(1, plan.slots)
    row = VMEM((8, plan.slots_pad), I32)
    whole = pl.BlockSpec(memory_space=VMEM)

    def over_freq(values):
        moved = {
            k: lax.ppermute(values[k], "freq", [(i, i ^ k) for i in range(freq)])
            for k in range(freq - 1, 0, -1)
        }
        return [values[0], *moved.values()]

    def to_piece(value, k):
        pairs = [(2 * z + h, 2 * (z ^ k) + h) for z in range(pieces) for h in range(2)]
        return lax.ppermute(value, "param", pairs)

    def to_core(value):
        return lax.ppermute(value, "param", [(i, i ^ 1) for i in range(plan.param)])

    ends = [g for g in (plan.groups - 2, plan.groups - 1, plan.groups) if g > 0]
    ranges = list(zip([0, *ends], ends))
    sizes = [end - begin for begin, end in ranges]
    totals = [min(end * plan.group, plan.here) - begin * plan.group for begin, end in ranges]
    block = (2, plan.sensors, plan.depth)
    early = min(totals[0] // CHUNK, EARLY) * CHUNK

    spectra = call(
        functools.partial(forward_kernel, plan),
        [shape((2 * plan.count, plan.mine, LANES), BF16)] * freq,
        (bins, jnp.transpose(sources, (0, 2, 1)), high, low),
        in_specs=[pl.BlockSpec(memory_space=pltpu.HBM)] * 4,
        scratch=[
            VMEM(bins.shape, I32),
            VMEM((plan.count, plan.mine, plan.steps), F32),
            VMEM(high.shape, BF16),
            VMEM(low.shape, BF16),
            row,
            VMEM((plan.count * plan.mine, pieces * plan.span_pad), F32),
            VMEM((freq, 2 * plan.count, plan.mine, LANES), BF16),
            pltpu.SemaphoreType.DMA((4,)),
        ],
        cost=cost(2 * 10**9, 2 * high.size),
        limit=FULL - ROOM,
    )
    arrived = over_freq(spectra)

    hbm = pl.BlockSpec(memory_space=pltpu.HBM)
    ready, hits = call(
        functools.partial(load_kernel, plan, early),
        [shape((early, *block), BF16), shape((freq, plan.bins, LANES), BF16)],
        (spectra[0], bins, kernel),
        in_specs=[pl.BlockSpec(memory_space=pl.ANY), whole, hbm],
        scratch=[row, pltpu.SemaphoreType.DMA((-(-early // CHUNK),))],
        cost=cost(4 * 10**9, 4 * early * plan.sensors * plan.depth),
    )
    ready = [ready]
    def join(at, last):
        groups = [sizes[i] for i in at]
        rows = (sum(groups) - last) * plan.block_pad + last * plan.fold_rows
        return call(
            functools.partial(join_kernel, plan, groups, last),
            [shape((rows, LANES), BF16)] * freq,
            [array for i in at for array in pairs[2 * i : 2 * i + 2]],
        )

    pairs = []
    for index, (begin, end) in enumerate(ranges):
        total, held = totals[index], [array.shape[0] for array in ready]
        rest = total - sum(held)
        ahead = min(totals[index + 1], AHEAD * CHUNK) if index + 1 < len(totals) else 0
        streams = int(rest > 0 or ahead > 0)
        size = shape((freq * sizes[index] * plan.block_pad, LANES), F32)
        own, other, *later = call(
            functools.partial(response_kernel, plan, begin, end, held, ahead),
            [size, size] + ([shape((ahead, *block), BF16)] if ahead else []),
            (*arrived, *ready) + (kernel,) * streams,
            in_specs=[whole] * (freq + len(ready)) + [hbm] * streams,
            scratch=[
                VMEM((max(rest, CHUNK), *block), BF16),
                VMEM((2 * plan.count, plan.depth, LANES), BF16),
                VMEM((end - begin, 2 * plan.depth, 2 * LANES), BF16),
                pltpu.SemaphoreType.DMA((-(-rest // CHUNK) + -(-ahead // CHUNK) + 1,)),
            ],
            cost=cost(total * 512 * plan.sensors * plan.depth, 4 * total * plan.sensors * plan.depth),
        )
        ready = later
        pairs += [own, to_core(other)]
        if index == len(ranges) - 2:
            joined, ready = lax.optimization_barrier((join([0], 0), ready))
            parts = over_freq(joined)
    parts += over_freq(join(list(range(1, len(sizes))), 1))

    partial = call(
        functools.partial(inverse_kernel, plan),
        [shape((plan.base, plan.span_pad), BF16 if k else F32) for k in range(pieces)],
        (hits, high, low, *parts),
        scratch=[
            VMEM((plan.comps * plan.block_pad, freq * LANES), BF16),
        ],
    )
    received = [to_piece(partial[k], k) for k in range(pieces - 1, 0, -1)]
    piece = call(sum_kernel, shape((plan.base, plan.span_pad), BF16), (partial[0], *received))
    mine = [piece] + [to_piece(piece, k) for k in range(1, pieces)]
    mine = call(stack_kernel, shape((pieces * plan.base, plan.span_pad), BF16), mine)
    theirs = to_core(mine)
    ours, pick = call(
        functools.partial(time_kernel, plan),
        [
            shape((plan.rows, plan.steps), F32),
            shape((plan.steps, pieces * plan.span_pad), BF16),
        ],
        (mine,),
        cost=cost(10**9, 10**6),
    )
    by_sensor = call(
        functools.partial(output_kernel, plan),
        shape((plan.block, plan.count, plan.steps), F32),
        (ours, theirs, pick),
    )
    return jnp.transpose(by_sensor, (1, 2, 0))


def solution(mesh):
    return jax.shard_map(
        functools.partial(shards, mesh),
        mesh=mesh,
        in_specs=(P(None, None, ("param", "freq")), P("freq", None, None, "param"), P()),
        out_specs=P(None, None, "freq"),
        check_vma=False,
    )
```
